32 devices in a mesh: dp: 8 (over z, x), mp: 4 (over y, core).
Axes of the slice: x: 2, y: 2, z: 4, core: 2. Of those that a mesh axis runs over, the one named last changes fastest.
Arguments:
- latents: bfloat16 [16, 8, 32, 16], P('dp'), may hold values from -6 to 6
- gaussian_noise: float32 [16, 8, 32, 16], P('dp'), may hold values from -6 to 6
- timesteps: int32 [16], P('dp'), may hold values from 2 to 999, as said below
- counts: int32 [8], P('dp'), may hold values from 256 to 512, as said below
- captions: bfloat16 [16, 120, 4096], P('dp'), may hold values from -6 to 6
- w_in: float32 [20, 1152, 1152], P(None, 'dp'), may hold values from -0.1875 to 0.1875
- w_out: float32 [8, 1152, 1152], P(None, 'dp'), may hold values from -0.1875 to 0.1875
- w_cap: float32 [4096, 1152], P('dp'), may hold values from -0.09375 to 0.09375
- w_small: float32 [312, 1152], replicated, may hold values from -0.1875 to 0.1875
- rows_in: float32 [20, 1152], P(None, 'dp'), may hold values from 0 to 1
- cols_in: float32 [20, 1152], replicated, may hold values from 0 to 1
- rows_out: float32 [8, 1152], P(None, 'dp'), may hold values from 0 to 1
- cols_out: float32 [8, 1152], replicated, may hold values from 0 to 1
- rows_cap: float32 [4096], P('dp'), may hold values from 0 to 1
- cols_cap: float32 [1152], replicated, may hold values from 0 to 1
- rows_small: float32 [312], replicated, may hold values from 0 to 1
- cols_small: float32 [1152], replicated, may hold values from 0 to 1
Outputs:
- loss_mean: float32 [], replicated
- new_in: float32 [20, 1152, 1152], P(None, 'dp')
- copy_in: bfloat16 [20, 1152, 1152], P(None, 'dp')
- update_in: float32 [20, 1152, 1152], P(None, 'dp')
- new_rows_in: float32 [20, 1152], P(None, 'dp')
- new_cols_in: float32 [20, 1152], replicated
- new_out: float32 [8, 1152, 1152], P(None, 'dp')
- copy_out: bfloat16 [8, 1152, 1152], P(None, 'dp')
- update_out: float32 [8, 1152, 1152], P(None, 'dp')
- new_rows_out: float32 [8, 1152], P(None, 'dp')
- new_cols_out: float32 [8, 1152], replicated
- new_cap: float32 [4096, 1152], P('dp')
- copy_cap: bfloat16 [4096, 1152], P('dp')
- update_cap: float32 [4096, 1152], P('dp')
- new_rows_cap: float32 [4096], P('dp')
- new_cols_cap: float32 [1152], replicated
- new_small: float32 [312, 1152], replicated
- copy_small: bfloat16 [312, 1152], replicated
- update_small: float32 [312, 1152], replicated
- new_rows_small: float32 [312], replicated
- new_cols_small: float32 [1152], replicated
- spreads: float32 [30], replicated
The draws below stay inside these ranges and needn't reach their ends.
Inputs may be any that keep to these rules, and one draw needn't show every extreme that they name: The samples of group g (rows g * 2 to g * 2 + 1) have timesteps from 2 + g * 124 to 1 + (g + 1) * 124. Each count is a multiple of 256; slots beyond counts are padding; some group is full and some holds one sample.
All inputs are finite; a program needn't handle non-finite values.
Results may differ from the reference program's by a relative error of at most 0.018.
The reference program's roundings to bfloat16 on the way count: a program that leaves them out, or rounds other values in their place, can miss the bound.
Values may be sent and summed in bfloat16 or wider, within the bound.
A program may use at most 320 MiB of HBM per device.

```python
import math
import jax
import jax.numpy as jnp
from jax import lax

HEADS = 16
HEAD_DIM = 72
D = 1152
FREQ = 256
CAP_DIM = 4096
CAP_LEN = 120
FRAMES = 8
GRID_H = 4
GRID_W = 8
PATCHES = 32
SLOTS = 2
STEP = 20
SAMPLES = 16
TOK_DEV = 512
ROWS_SMALL = 312
N_DP = 8


def draw_timesteps(key, part):
    bin_width = 998 // N_DP
    group_index = jnp.arange(N_DP * SLOTS, dtype=jnp.int32) // SLOTS
    return 2 + group_index * bin_width + jax.random.randint(key, (N_DP * SLOTS,), 0, bin_width, dtype=jnp.int32)


def draw_counts(key, part):
    key_count, key_full, key_single = jax.random.split(key, 3)
    samples = jax.random.randint(key_count, (N_DP,), 1, SLOTS + 1, dtype=jnp.int32)
    full_at = jax.random.randint(key_full, (), 0, N_DP, dtype=jnp.int32)
    single_at = (full_at + 1 + jax.random.randint(key_single, (), 0, N_DP - 1, dtype=jnp.int32)) % N_DP
    group_index = jnp.arange(N_DP, dtype=jnp.int32)
    samples = jnp.where(group_index == full_at, SLOTS, jnp.where(group_index == single_at, 1, samples))
    return samples * (FRAMES * PATCHES)


def stat_draw(key, shape, tag):
    own_key = jax.random.fold_in(key, tag)
    estimate = 0.0001 / (SLOTS * FRAMES * GRID_H * GRID_W * N_DP)
    factor = jnp.exp(jax.random.uniform(own_key, shape, jnp.float32, math.log(0.5), math.log(1.5)))
    return 0.1 * estimate * factor


def draw_rows_in(key, part):
    return stat_draw(key, (20, D), 101)


def draw_cols_in(key, part):
    return stat_draw(key, (20, D), 202)


def draw_rows_out(key, part):
    return stat_draw(key, (8, D), 303)


def draw_cols_out(key, part):
    return stat_draw(key, (8, D), 404)


def draw_rows_cap(key, part):
    return stat_draw(key, (CAP_DIM,), 505)


def draw_cols_cap(key, part):
    return stat_draw(key, (D,), 606)


def draw_rows_small(key, part):
    return stat_draw(key, (56 + FREQ,), 707)


def draw_cols_small(key, part):
    return stat_draw(key, (D,), 808)


def block_levels(rng, extent, cuts, least, high):
    loudness = 1.0
    for axis_at, parts in cuts:
        draws = jax.random.uniform(jax.random.fold_in(jax.random.fold_in(rng, 6), axis_at), (parts,), jnp.float32, least / len(cuts), high / len(cuts))
        loudness = loudness * jnp.repeat(jnp.exp(draws), extent[axis_at] // parts).reshape((-1,) + (1,) * (len(extent) - 1 - axis_at))
    return loudness


def normal_values(key, extent, deviation, limit, pieces=(), kind=jnp.bfloat16):
    result = deviation * jax.random.normal(key, extent, jnp.float32)
    if pieces:
        result = result * block_levels(key, extent, pieces, -0.22, 0.18)
    return jnp.clip(result, -limit, limit).astype(kind)


def setup_inputs(seed: int = 0) -> dict:
    streams_of = jax.random.split(jax.random.key(seed), 18)
    return {
        "latents": normal_values(streams_of[0], (SAMPLES, FRAMES, PATCHES, 16), 1.0, 6.0, ((0, 8),)),
        "gaussian_noise": normal_values(streams_of[1], (SAMPLES, FRAMES, PATCHES, 16), 1.0, 6.0, ((0, 8),), jnp.float32),
        "timesteps": draw_timesteps(jax.random.fold_in(streams_of[17], 71), 0),
        "counts": draw_counts(jax.random.fold_in(streams_of[17], 71), 0),
        "captions": normal_values(streams_of[4], (SAMPLES, CAP_LEN, CAP_DIM), 1.0, 6.0, ((0, 8),)),
        "w_in": normal_values(streams_of[5], (20, D, D), D ** -0.5, 0.1875, ((1, 8),), jnp.float32),
        "w_out": normal_values(streams_of[6], (8, D, D), D ** -0.5, 0.1875, ((1, 8),), jnp.float32),
        "w_cap": normal_values(streams_of[7], (CAP_DIM, D), CAP_DIM ** -0.5, 0.09375, ((0, 8),), jnp.float32),
        "w_small": normal_values(streams_of[8], (ROWS_SMALL, D), D ** -0.5, 0.1875, (), jnp.float32),
        "rows_in": draw_rows_in(jax.random.fold_in(streams_of[17], 71), 0),
        "cols_in": draw_cols_in(jax.random.fold_in(streams_of[17], 71), 0),
        "rows_out": draw_rows_out(jax.random.fold_in(streams_of[17], 71), 0),
        "cols_out": draw_cols_out(jax.random.fold_in(streams_of[17], 71), 0),
        "rows_cap": draw_rows_cap(jax.random.fold_in(streams_of[17], 71), 0),
        "cols_cap": draw_cols_cap(jax.random.fold_in(streams_of[17], 71), 0),
        "rows_small": draw_rows_small(jax.random.fold_in(streams_of[17], 71), 0),
        "cols_small": draw_cols_small(jax.random.fold_in(streams_of[17], 71), 0),
    }


@jax.custom_vjp
def low(v):
    return lax.optimization_barrier(v.astype(jnp.bfloat16)).astype(jnp.float32)

@jax.custom_vjp
def low_back(v):
    return v

def low_keep(v):
    return (low(v), None)

def low_pass(kept, grad):
    return (grad,)

def back_keep(v):
    return (v, None)

def back_low(kept, grad):
    return (low(grad),)
low.defvjp(low_keep, low_pass)
low_back.defvjp(back_keep, back_low)
highest = lax.Precision.HIGHEST
norm_eps = 1e-06
relative_rate = 0.5
tanh_coeff = math.sqrt(2.0 / math.pi)
angle_unit = math.pi / 2.0 / 1.008 / 1000.0

def matmul(left, right):
    return jnp.dot(left, right, precision=highest, preferred_element_type=jnp.float32)

def einsum_hi(form, left, right):
    return jnp.einsum(form, left, right, precision=highest, preferred_element_type=jnp.float32)

def both_round(values):
    return low(low_back(values))

def gelu_tanh(values):
    return 0.5 * values * (1.0 + jnp.tanh(tanh_coeff * (values + 0.044715 * values * values * values)))

def layer_norm(values):
    center = values - lax.optimization_barrier(jnp.mean(values, axis=-1, keepdims=True))
    return center * lax.rsqrt(lax.optimization_barrier(jnp.mean(center * center, axis=-1, keepdims=True)) + norm_eps)

def modulate(hidden, shift_rows, scale_rows):
    return layer_norm(hidden) * (1.0 + scale_rows) + shift_rows

def sincos(positions, table_width):
    half_width = table_width // 2
    frequency = jnp.exp(-math.log(10000.0) * jnp.arange(half_width).astype(jnp.float32) / half_width)
    angles = positions[:, None] * frequency[None, :]
    return jnp.concatenate([jnp.sin(angles), jnp.cos(angles)], axis=1)

def position_tables():
    patch_index = jnp.arange(GRID_H * GRID_W)
    spatial = jnp.concatenate([sincos((patch_index // GRID_W).astype(jnp.float32), D // 2), sincos((patch_index % GRID_W).astype(jnp.float32), D // 2)], axis=1)
    temporal = sincos(jnp.arange(FRAMES).astype(jnp.float32), D)
    return (spatial, temporal)

def time_features(timesteps):
    half_width = FREQ // 2
    frequency = jnp.exp(-math.log(10000.0) * jnp.arange(half_width).astype(jnp.float32) / half_width)
    angles = timesteps.astype(jnp.float32)[:, None] * frequency[None, :]
    return jnp.concatenate([jnp.cos(angles), jnp.sin(angles)], axis=1)

def plan(timesteps):
    moment = timesteps.astype(jnp.float32)
    start_angle = 8.0 * angle_unit
    cos_start = math.cos(start_angle) ** 2
    remain_now = jnp.sin((1000.0 - moment) * angle_unit)
    remain_before = jnp.sin((1001.0 - moment) * angle_unit)
    alpha_now = remain_now * remain_now / cos_start
    alpha_before = remain_before * remain_before / cos_start
    rest_now = jnp.sin(2.0 * start_angle + moment * angle_unit) * jnp.sin(moment * angle_unit) / cos_start
    rest_before = jnp.sin(2.0 * start_angle + (moment - 1.0) * angle_unit) * jnp.sin((moment - 1.0) * angle_unit) / cos_start
    beta_now = jnp.sin(2.0 * start_angle + (2.0 * moment - 1.0) * angle_unit) * math.sin(angle_unit) / (remain_before * remain_before)
    posterior = beta_now * rest_before / rest_now
    kappa = beta_now * beta_now * alpha_before / (rest_now * alpha_now)
    return (alpha_now, rest_now, beta_now, posterior, kappa)

def patch_terms(output, target, squared, beta_rows, posterior_rows, kappa_rows):
    error_rows = output[:, :, 0:4] - target
    log_beta = jnp.log(beta_rows)[:, None, None]
    log_post = jnp.log(posterior_rows)[:, None, None]
    fraction = (output[:, :, 4:8] + 1.0) * 0.5
    log_model = fraction * log_beta + (1.0 - fraction) * log_post
    diverge = 0.5 * (-1.0 + log_model - log_post + jnp.exp(log_post - log_model) + kappa_rows[:, None, None] * squared * jnp.exp(-log_model))
    return lax.optimization_barrier(jnp.mean(error_rows * error_rows, axis=(1, 2))) + lax.optimization_barrier(jnp.mean(diverge, axis=(1, 2))) / math.log(2.0)

def to_frames(stacked, head_count):
    leading = stacked.shape[0]
    return stacked.reshape(leading, SLOTS, FRAMES, PATCHES, head_count, HEAD_DIM).transpose(0, 1, 3, 2, 4, 5).reshape(leading, SLOTS * PATCHES, FRAMES, head_count, HEAD_DIM)

def from_frames(stacked, head_count):
    leading = stacked.shape[0]
    return stacked.reshape(leading, SLOTS, PATCHES, FRAMES, head_count, HEAD_DIM).transpose(0, 1, 3, 2, 4, 5).reshape(leading, SLOTS * FRAMES * PATCHES, head_count * HEAD_DIM)

def attention(queries, key_rows, value_rows):
    scores = low_back(einsum_hi('bqhc,bkhc->bhqk', queries, key_rows) * HEAD_DIM ** (-0.5))
    weights = low(jax.nn.softmax(scores, axis=-1))
    return einsum_hi('bhqk,bkhc->bqhc', weights, value_rows)

def group_pass(params, one_item):
    w_in, w_out, w_cap, w_small = params
    latents, noise_rows, timesteps, captions, count, squared = one_item
    per_sample = FRAMES * PATCHES
    alpha_now, rest_now, beta_now, posterior, kappa = plan(timesteps)
    noisy_low = low(jnp.sqrt(alpha_now)[:, None, None, None] * latents + jnp.sqrt(rest_now)[:, None, None, None] * noise_rows)
    patches = noisy_low.reshape(TOK_DEV, 16)
    patch_w = w_small[0:16]
    freq_w = w_small[16:16 + FREQ]
    tables = w_small[16 + FREQ:24 + FREQ]
    final_w = w_small[24 + FREQ:]
    temb_w = w_in[19]
    spatial_pos, temporal_pos = position_tables()
    embedded = low_back(matmul(patches, patch_w))
    hidden = (embedded.reshape(SLOTS, FRAMES, PATCHES, D) + spatial_pos[None, None]).reshape(SLOTS, per_sample, D)
    first_pre = low_back(matmul(low(time_features(timesteps)), freq_w))
    time_emb = low_back(matmul(low(jax.nn.silu(first_pre)), temb_w))
    modulation = low_back(einsum_hi('sd,kde->ske', low(jax.nn.silu(time_emb)), w_in[13:19])) + tables[None, 0:6]
    shift_a, scale_a, gate_a, shift_b, scale_b, gate_b = [modulation[:, number][:, None, :] for number in range(6)]
    cap_mid = low_back(matmul(captions.reshape(SLOTS * CAP_LEN, CAP_DIM), w_cap))
    context = both_round(matmul(low(gelu_tanh(cap_mid)), w_out[7].T))
    normed_a = low(modulate(hidden, shift_a, scale_a)).reshape(TOK_DEV, D)
    stacked = both_round(einsum_hi('td,kde->kte', normed_a, w_in[0:3])).reshape(3, SLOTS * FRAMES, PATCHES, HEADS, HEAD_DIM)
    mixed_rows = both_round(attention(stacked[0], stacked[1], stacked[2])).reshape(TOK_DEV, D)
    hidden = hidden + gate_a * low_back(matmul(mixed_rows, w_out[0].T)).reshape(SLOTS, per_sample, D)
    timed_low = low(hidden.reshape(SLOTS, FRAMES, PATCHES, D) + temporal_pos[None, :, None, :]).reshape(TOK_DEV, D)
    stacked = to_frames(both_round(einsum_hi('td,kde->kte', timed_low, w_in[3:6])), HEADS)
    mixed_rows = both_round(from_frames(attention(stacked[0], stacked[1], stacked[2])[None], HEADS)[0])
    hidden = hidden + gate_a * low_back(matmul(mixed_rows, w_out[1].T)).reshape(SLOTS, per_sample, D)
    queries = both_round(matmul(low(hidden).reshape(TOK_DEV, D), w_in[6])).reshape(SLOTS, per_sample, HEADS, HEAD_DIM)
    key_value = both_round(einsum_hi('rd,kde->kre', context, w_in[7:9])).reshape(2, SLOTS, CAP_LEN, HEADS, HEAD_DIM)
    mixed_rows = both_round(attention(queries, key_value[0], key_value[1])).reshape(TOK_DEV, D)
    hidden = hidden + low_back(matmul(mixed_rows, w_out[2].T)).reshape(SLOTS, per_sample, D)
    normed_b = low(modulate(hidden, shift_b, scale_b)).reshape(TOK_DEV, D)
    inner_pre = low_back(einsum_hi('td,kde->tke', normed_b, w_in[9:13]))
    branch = low_back(einsum_hi('tke,kde->td', low(gelu_tanh(inner_pre)), w_out[3:7]))
    hidden = hidden + gate_b * branch.reshape(SLOTS, per_sample, D)
    shift_f = (tables[6] + time_emb)[:, None, :]
    scale_f = (tables[7] + time_emb)[:, None, :]
    normed_f = low(modulate(hidden, shift_f, scale_f)).reshape(TOK_DEV, D)
    output = low_back(einsum_hi('td,od->to', normed_f, final_w)).reshape(TOK_DEV, 4, 8)
    target = noise_rows.reshape(TOK_DEV, 4, 4)
    live_rows = jnp.repeat((jnp.arange(SLOTS) * per_sample < count).astype(jnp.float32), per_sample)
    terms = patch_terms(output, target, squared, jnp.repeat(beta_now, per_sample), jnp.repeat(posterior, per_sample), jnp.repeat(kappa, per_sample))
    return (jnp.sum(terms * live_rows), output[:, :, 0:4] - target)

def adafactor(weight, grad, row_stats, col_stats):
    rho = 1.0 - STEP ** (-0.8)
    square = grad * grad + 1e-30
    rows_new = rho * row_stats + (1.0 - rho) * lax.optimization_barrier(jnp.mean(square, axis=-1))
    cols_new = rho * col_stats + (1.0 - rho) * lax.optimization_barrier(jnp.mean(square, axis=-2))
    second = rows_new[..., :, None] * cols_new[..., None, :] / lax.optimization_barrier(jnp.mean(rows_new, axis=-1))[..., None, None]
    update = grad * lax.rsqrt(second)
    spread = jnp.sqrt(lax.optimization_barrier(jnp.mean(update * update, axis=(-2, -1))))
    clipped = update / jnp.maximum(1.0, spread)[..., None, None]
    weight_scale = jnp.sqrt(lax.optimization_barrier(jnp.mean(weight * weight, axis=(-2, -1))))
    new_weight = weight - relative_rate * weight_scale[..., None, None] * clipped
    return (new_weight, new_weight.astype(jnp.bfloat16), clipped, rows_new, cols_new, spread.reshape(-1))

def reference(latents, gaussian_noise, timesteps, counts, captions, w_in, w_out, w_cap, w_small, rows_in, cols_in, rows_out, cols_out, rows_cap, cols_cap, rows_small, cols_small):
    group_data = (latents.astype(jnp.float32).reshape(N_DP, SLOTS, FRAMES, PATCHES, 16), gaussian_noise.reshape(N_DP, SLOTS, FRAMES, PATCHES, 16), timesteps.reshape(N_DP, SLOTS), captions.astype(jnp.float32).reshape(N_DP, SLOTS, CAP_LEN, CAP_DIM), counts)

    def run(params, squared):
        rounded = tuple((low(weight) for weight in params))

        def one_group(one_item):
            return group_pass(rounded, one_item)
        losses, errors = lax.map(jax.checkpoint(one_group), group_data + (squared,))
        return (jnp.sum(losses), errors)
    params = (w_in, w_out, w_cap, w_small)
    errors = run(params, jnp.zeros((N_DP, TOK_DEV, 4, 4), jnp.float32))[1]
    squared = errors * errors
    total_sum, pullback = jax.vjp(lambda weights: run(weights, squared)[0], params)
    gradients = pullback(jnp.ones_like(total_sum))[0]
    patches_all = jnp.sum(counts).astype(jnp.float32)
    in_new, in_copy, in_update, in_rows, in_cols, in_spread = adafactor(w_in, gradients[0] / patches_all, rows_in, cols_in)
    out_new, out_copy, out_update, out_rows, out_cols, out_spread = adafactor(w_out, gradients[1] / patches_all, rows_out, cols_out)
    cap_new, cap_copy, cap_update, cap_rows, cap_cols, cap_spread = adafactor(w_cap, gradients[2] / patches_all, rows_cap, cols_cap)
    small_new, small_copy, small_update, small_rows, small_cols, small_spread = adafactor(w_small, gradients[3] / patches_all, rows_small, cols_small)
    spreads = jnp.concatenate([in_spread, out_spread, cap_spread, small_spread])
    return (total_sum / patches_all, in_new, in_copy, in_update, in_rows, in_cols, out_new, out_copy, out_update, out_rows, out_cols, cap_new, cap_copy, cap_update, cap_rows, cap_cols, small_new, small_copy, small_update, small_rows, small_cols, spreads)
```

```python
import math

import jax
import jax.numpy as jnp
from jax import lax
from jax.sharding import PartitionSpec as P

HEAD_DIM = 72
D = 1152
FREQ = 256
CAP_DIM = 4096
CAP_LEN = 120
FRAMES = 8
GRID_H = 4
GRID_W = 8
PATCHES = 32
SLOTS = 2
STEP = 20
TOK_DEV = 512
CAP_PAD = 128


norm_eps = 1e-06
relative_rate = 0.5
tanh_coeff = math.sqrt(2.0 / math.pi)
angle_unit = math.pi / 2.0 / 1.008 / 1000.0


def product(left, right):
    return jnp.dot(left, right, preferred_element_type=jnp.float32)


def contract(form, left, right):
    return jnp.einsum(form, left, right, preferred_element_type=jnp.float32)


def gelu_tanh(values):
    return (
        0.5 * values * (1.0 + jnp.tanh(tanh_coeff * (values + 0.044715 * values * values * values)))
    )


def layer_norm(values):
    center = values - jnp.mean(values, axis=-1, keepdims=True)
    return center * lax.rsqrt(jnp.mean(center * center, axis=-1, keepdims=True) + norm_eps)


def modulate(hidden, shift_rows, scale_rows):
    return layer_norm(hidden) * (1.0 + scale_rows) + shift_rows


def modulate_grad(hidden, shift_rows, scale_rows, grad_rows):
    pullback = jax.vjp(modulate, hidden, shift_rows, scale_rows)[1]
    return pullback(grad_rows)


def act_grad(function, values, grad_rows):
    return jax.vjp(function, values)[1](grad_rows)[0]


def sincos(positions, table_width):
    half_width = table_width // 2
    frequency = jnp.exp(
        -math.log(10000.0) * jnp.arange(half_width).astype(jnp.float32) / half_width
    )
    angles = positions[:, None] * frequency[None, :]
    return jnp.concatenate([jnp.sin(angles), jnp.cos(angles)], axis=1)


def position_tables():
    patch_index = jnp.arange(GRID_H * GRID_W)
    spatial = jnp.concatenate(
        [
            sincos((patch_index // GRID_W).astype(jnp.float32), D // 2),
            sincos((patch_index % GRID_W).astype(jnp.float32), D // 2),
        ],
        axis=1,
    )
    temporal = sincos(jnp.arange(FRAMES).astype(jnp.float32), D)
    return (spatial, temporal)


def time_features(timesteps):
    half_width = FREQ // 2
    frequency = jnp.exp(
        -math.log(10000.0) * jnp.arange(half_width).astype(jnp.float32) / half_width
    )
    angles = timesteps.astype(jnp.float32)[:, None] * frequency[None, :]
    return jnp.concatenate([jnp.cos(angles), jnp.sin(angles)], axis=1)


def plan(timesteps):
    moment = timesteps.astype(jnp.float32)
    start_angle = 8.0 * angle_unit
    cos_start = math.cos(start_angle) ** 2
    remain_now = jnp.sin((1000.0 - moment) * angle_unit)
    remain_before = jnp.sin((1001.0 - moment) * angle_unit)
    alpha_now = remain_now * remain_now / cos_start
    alpha_before = remain_before * remain_before / cos_start
    rest_now = (
        jnp.sin(2.0 * start_angle + moment * angle_unit) * jnp.sin(moment * angle_unit) / cos_start
    )
    rest_before = (
        jnp.sin(2.0 * start_angle + (moment - 1.0) * angle_unit)
        * jnp.sin((moment - 1.0) * angle_unit)
        / cos_start
    )
    beta_now = (
        jnp.sin(2.0 * start_angle + (2.0 * moment - 1.0) * angle_unit)
        * math.sin(angle_unit)
        / (remain_before * remain_before)
    )
    posterior = beta_now * rest_before / rest_now
    kappa = beta_now * beta_now * alpha_before / (rest_now * alpha_now)
    return (alpha_now, rest_now, beta_now, posterior, kappa)


def patch_terms(output, target, squared, beta_rows, posterior_rows, kappa_rows):
    error_rows = output[:, :, 0:4] - target
    log_beta = jnp.log(beta_rows)[:, None, None]
    log_post = jnp.log(posterior_rows)[:, None, None]
    fraction = (output[:, :, 4:8] + 1.0) * 0.5
    log_model = fraction * log_beta + (1.0 - fraction) * log_post
    diverge = 0.5 * (
        -1.0
        + log_model
        - log_post
        + jnp.exp(log_post - log_model)
        + kappa_rows[:, None, None] * squared * jnp.exp(-log_model)
    )
    return jnp.mean(error_rows * error_rows, axis=(1, 2)) + jnp.mean(
        diverge, axis=(1, 2)
    ) / math.log(2.0)


def to_frames(stacked, head_count):
    leading = stacked.shape[0]
    return (
        stacked.reshape(leading, SLOTS, FRAMES, PATCHES, head_count, HEAD_DIM)
        .transpose(0, 1, 3, 2, 4, 5)
        .reshape(leading, SLOTS * PATCHES, FRAMES, head_count, HEAD_DIM)
    )


def from_frames(stacked, head_count):
    leading = stacked.shape[0]
    return (
        stacked.reshape(leading, SLOTS, PATCHES, FRAMES, head_count, HEAD_DIM)
        .transpose(0, 1, 3, 2, 4, 5)
        .reshape(leading, SLOTS * FRAMES * PATCHES, head_count * HEAD_DIM)
    )


def attend_forward(queries, key_rows, value_rows):
    scores = contract("bqhc,bkhc->bhqk", queries, key_rows) * HEAD_DIM ** (-0.5)
    highest = jnp.max(scores, axis=-1, keepdims=True)
    shifted = jnp.exp(scores - highest)
    denominator = jnp.sum(shifted, axis=-1, keepdims=True)
    weights = (shifted / denominator).astype(jnp.bfloat16)
    return (contract("bhqk,bkhc->bqhc", weights, value_rows), highest + jnp.log(denominator))


def attend_backward(queries, key_rows, value_rows, logsum, grad_mixed):
    scores = contract("bqhc,bkhc->bhqk", queries, key_rows) * HEAD_DIM ** (-0.5)
    probability = jnp.exp(scores - logsum)
    grad_value = contract("bhqk,bqhc->bkhc", probability.astype(jnp.bfloat16), grad_mixed)
    grad_prob = contract("bqhc,bkhc->bhqk", grad_mixed, value_rows)
    grad_scores = (
        probability * (grad_prob - jnp.sum(probability * grad_prob, axis=-1, keepdims=True))
    ).astype(jnp.bfloat16)
    grad_query = contract("bhqk,bkhc->bqhc", grad_scores, key_rows) * HEAD_DIM ** (-0.5)
    grad_key = contract("bhqk,bqhc->bkhc", grad_scores, queries) * HEAD_DIM ** (-0.5)
    return (grad_query, grad_key, grad_value)


def new_stat(old_stat, sums, length, inverse_sq):
    rho = 1.0 - STEP ** (-0.8)
    return rho * old_stat + (1.0 - rho) * (sums * inverse_sq / length + 1e-30)


def ratio_terms(weight, grad, rows_new, cols_new):
    ratio = jnp.sum(grad * grad / (rows_new[:, :, None] * cols_new[:, None, :]), axis=(1, 2))
    return jnp.stack([jnp.sum(rows_new, axis=1), ratio, jnp.sum(weight * weight, axis=(1, 2))])


def apply_update(weight, grad, rows_new, cols_new, mean_rows, spread, weight_scale):
    second = rows_new[:, :, None] * cols_new[:, None, :] / mean_rows[:, None, None]
    update = grad * lax.rsqrt(second)
    clipped = update / jnp.maximum(1.0, spread)[:, None, None]
    new_weight = weight - relative_rate * weight_scale[:, None, None] * clipped
    return (new_weight, new_weight.astype(jnp.bfloat16), clipped)


def token_sum(pieces):
    return lax.psum_scatter(
        pieces.astype(jnp.bfloat16), "mp", scatter_dimension=0, tiled=True
    ).astype(jnp.float32)


def token_gather(rows):
    return lax.all_gather(rows, "mp", axis=0, tiled=True)


def pad_samples(rows):
    stacked = rows.reshape(SLOTS, CAP_LEN, rows.shape[1])
    padded = jnp.pad(stacked, ((0, 0), (0, CAP_PAD - CAP_LEN), (0, 0)))
    return padded.reshape(SLOTS * CAP_PAD, rows.shape[1])


def cut_samples(rows):
    stacked = rows.reshape(SLOTS, CAP_PAD, rows.shape[1])[:, 0:CAP_LEN]
    return stacked.reshape(SLOTS * CAP_LEN, rows.shape[1])


def side_by_side(stacked):
    return stacked.transpose(1, 0, 2).reshape(stacked.shape[1], -1)


def heads_of(rows, lead, count):
    return rows.reshape(*lead, count, HEAD_DIM)


def spatial_heads(rows, count):
    return rows.reshape(SLOTS * FRAMES, PATCHES, count, HEAD_DIM)


def temporal_heads(rows, count):
    return to_frames(rows[None], count)[0]


def shards(
    latents, gaussian_noise, timesteps, counts, captions,
    w_in, w_out, w_cap, w_small,
    rows_in, cols_in, rows_out, cols_out, rows_cap, cols_cap, rows_small, cols_small,
):
    bfloat = jnp.bfloat16
    mp_index = lax.axis_index("mp")
    dp_index = lax.axis_index("dp")
    mp_size = lax.axis_size("mp")
    dp_size = lax.axis_size("dp")
    local_width = w_in.shape[2] // mp_size
    head_count = local_width // HEAD_DIM
    col_start = mp_index * local_width
    row_count_own = w_in.shape[1]
    row_start = dp_index * row_count_own
    cap_rows_own = w_cap.shape[0]
    small_rows = 56 + FREQ
    per_sample = FRAMES * PATCHES
    own_tokens = TOK_DEV // mp_size
    token_start = mp_index * own_tokens
    sample = token_start // per_sample
    wide = 4 * local_width
    lw = local_width

    in_cols = lax.dynamic_slice_in_dim(w_in[0:13], col_start, lw, 2).astype(bfloat)
    out_cols = lax.dynamic_slice_in_dim(w_out, col_start, lw, 2).astype(bfloat)
    cap_cols = lax.dynamic_slice_in_dim(w_cap, col_start, lw, 1).astype(bfloat)
    pack_s = side_by_side(jnp.concatenate([in_cols[0:3], out_cols[0:1]], axis=0))
    pack_t = side_by_side(jnp.concatenate([in_cols[3:6], out_cols[1:2]], axis=0))
    pack_c = side_by_side(jnp.concatenate([in_cols[6:9], out_cols[2:3]], axis=0))
    pack_i = side_by_side(in_cols[9:13])
    pack_o = side_by_side(out_cols[3:7])
    pack_x = jnp.concatenate([cap_cols, out_cols[7]], axis=0)
    full_s = lax.all_gather(pack_s, "dp", axis=0, tiled=True)
    full_t = lax.all_gather(pack_t, "dp", axis=0, tiled=True)
    full_x = lax.all_gather(pack_x, "dp", axis=0, tiled=False)
    full_c = lax.all_gather(pack_c, "dp", axis=0, tiled=True)
    full_i = lax.all_gather(pack_i, "dp", axis=0, tiled=True)
    full_o = lax.all_gather(pack_o, "dp", axis=0, tiled=True)
    full_cap = full_x[:, 0:cap_rows_own].reshape(CAP_DIM, lw)
    full_c2 = full_x[:, cap_rows_own:].reshape(D, lw)
    mod_rows = w_in[13:19].astype(bfloat)
    temb_rows = w_in[19].astype(bfloat)

    full_small = w_small.astype(bfloat)
    patch_w = full_small[0:16]
    freq_w = full_small[16 : 16 + FREQ]
    tables = full_small[16 + FREQ : 24 + FREQ].astype(jnp.float32)
    final_w = full_small[24 + FREQ :]

    def own_rows(rows):
        return lax.dynamic_slice_in_dim(rows, token_start, own_tokens, 0)

    def own_cols(rows):
        return lax.dynamic_slice_in_dim(rows, row_start, row_count_own, 1)

    all_times = lax.all_gather(timesteps, "dp", axis=0, tiled=True)
    alpha_now, rest_now, beta_now, posterior, kappa = plan(timesteps)
    features = time_features(all_times).astype(bfloat)
    first_pre = product(features, freq_w)
    first_act = jax.nn.silu(first_pre).astype(bfloat)
    time_emb_all = lax.psum(product(own_cols(first_act), temb_rows), "dp")
    temb_act = jax.nn.silu(time_emb_all).astype(bfloat)
    mod_part = contract("sd,kde->ske", own_cols(temb_act), mod_rows)
    modulation = (
        lax.psum_scatter(mod_part, "dp", scatter_dimension=0, tiled=True) + tables[None, 0:6]
    )
    time_emb = lax.dynamic_slice_in_dim(time_emb_all, dp_index * SLOTS, SLOTS, 0)
    mods_own = lax.dynamic_index_in_dim(modulation, sample, 0, keepdims=False)
    shift_a, scale_a, gate_a, shift_b, scale_b, gate_b = [
        mods_own[number : number + 1] for number in range(6)
    ]
    temb_own = lax.dynamic_slice_in_dim(time_emb, sample, 1, 0)

    noisy_low = (
        jnp.sqrt(alpha_now)[:, None, None, None] * latents.astype(jnp.float32)
        + jnp.sqrt(rest_now)[:, None, None, None] * gaussian_noise
    ).astype(bfloat)
    patches = noisy_low.reshape(TOK_DEV, 16)
    spatial_pos, temporal_pos = position_tables()
    start_hidden = (
        product(patches, patch_w).reshape(SLOTS * FRAMES, PATCHES, D) + spatial_pos[None]
    ).reshape(SLOTS, per_sample, D)
    start_own = own_rows(start_hidden.reshape(TOK_DEV, D))

    cap_rows = captions.reshape(SLOTS * CAP_LEN, CAP_DIM)
    cap_mid = product(cap_rows, full_cap)
    cap_act = gelu_tanh(cap_mid).astype(bfloat)
    context_own = token_sum(pad_samples(contract("re,de->rd", cap_act, full_c2))).astype(bfloat)
    context_low = cut_samples(token_gather(context_own))

    normed_a = (
        modulate(start_hidden, modulation[:, 0][:, None], modulation[:, 1][:, None])
        .astype(bfloat)
        .reshape(TOK_DEV, D)
    )
    qkv = product(normed_a, full_s[:, 0 : 3 * lw]).astype(bfloat)
    qkv_s = [spatial_heads(qkv[:, k * lw : (k + 1) * lw], head_count) for k in range(3)]
    mixed_s, logsum_s = attend_forward(*qkv_s)
    mixed_s_low = mixed_s.astype(bfloat).reshape(TOK_DEV, lw)
    branch_s = token_sum(contract("te,de->td", mixed_s_low, full_s[:, 3 * lw :]))
    hidden_s = start_own + gate_a * branch_s
    frame_start = (token_start % per_sample) // PATCHES
    frames_own = own_tokens // PATCHES
    temporal_own = lax.dynamic_slice_in_dim(temporal_pos, frame_start, frames_own, 0)
    timed_own = (
        hidden_s.reshape(frames_own, PATCHES, D) + temporal_own[:, None, :]
    ).astype(bfloat)
    timed_low = token_gather(timed_own.reshape(own_tokens, D))
    qkv = product(timed_low, full_t[:, 0 : 3 * lw]).astype(bfloat)
    qkv_t = [temporal_heads(qkv[:, k * lw : (k + 1) * lw], head_count) for k in range(3)]
    mixed_t, logsum_t = attend_forward(*qkv_t)
    mixed_t_low = from_frames(mixed_t.astype(bfloat)[None], head_count)[0]
    branch_t = token_sum(contract("te,de->td", mixed_t_low, full_t[:, 3 * lw :]))
    hidden_t = hidden_s + gate_a * branch_t
    hidden_low = token_gather(hidden_t.astype(bfloat))
    query_c = (
        product(hidden_low, full_c[:, 0:lw])
        .astype(bfloat)
        .reshape(SLOTS, per_sample, head_count, HEAD_DIM)
    )
    key_value = product(context_low, full_c[:, lw : 3 * lw]).astype(bfloat)
    key_c = key_value[:, 0:lw].reshape(SLOTS, CAP_LEN, head_count, HEAD_DIM)
    value_c = key_value[:, lw:].reshape(SLOTS, CAP_LEN, head_count, HEAD_DIM)
    mixed_c, logsum_c = attend_forward(query_c, key_c, value_c)
    mixed_c_low = mixed_c.astype(bfloat).reshape(TOK_DEV, lw)
    hidden_c = hidden_t + token_sum(contract("te,de->td", mixed_c_low, full_c[:, 3 * lw :]))
    normed_b = token_gather(modulate(hidden_c, shift_b, scale_b).astype(bfloat))
    inner_pre = product(normed_b, full_i)
    inner_act = gelu_tanh(inner_pre).astype(bfloat)
    branch_m = token_sum(contract("te,de->td", inner_act, full_o))
    hidden_m = hidden_c + gate_b * branch_m
    shift_f = tables[6:7] + temb_own
    scale_f = tables[7:8] + temb_own
    normed_f = modulate(hidden_m, shift_f, scale_f).astype(bfloat)
    output = contract("td,od->to", normed_f, final_w).reshape(own_tokens, 4, 8)
    target = own_rows(gaussian_noise.reshape(TOK_DEV, 4, 4))
    error_rows = output[:, :, 0:4] - target
    squared = error_rows * error_rows
    live = (sample * per_sample < counts[0]).astype(jnp.float32)

    def of_sample(values):
        return jnp.broadcast_to(lax.dynamic_slice_in_dim(values, sample, 1, 0), (own_tokens,))

    beta_rows = of_sample(beta_now)
    posterior_rows = of_sample(posterior)
    kappa_rows = of_sample(kappa)

    def patch_loss(values):
        return jnp.sum(
            patch_terms(values, target, squared, beta_rows, posterior_rows, kappa_rows) * live
        )

    loss_local, loss_pull = jax.vjp(patch_loss, output)
    grad_output = loss_pull(jnp.ones_like(loss_local))[0].astype(bfloat).reshape(own_tokens, 32)
    grad_final = contract("to,td->od", grad_output, normed_f)
    grad_normed = contract("to,od->td", grad_output, final_w)
    grad_hidden, grad_shift_f, grad_scale_f = modulate_grad(hidden_m, shift_f, scale_f, grad_normed)
    grad_gate_b = jnp.sum(grad_hidden * branch_m, axis=0, keepdims=True)
    grad_branch = token_gather((gate_b * grad_hidden).astype(bfloat))
    grad_inner = act_grad(gelu_tanh, inner_pre, product(grad_branch, full_o)).astype(bfloat)
    part = contract("te,de->td", grad_inner, full_i)
    grad_pack_o = contract("td,te->de", grad_branch, inner_act)
    grad_pack_i = contract("td,te->de", normed_b, grad_inner)

    def row_sum(pieces):
        return lax.psum_scatter(
            pieces.astype(bfloat), "dp", scatter_dimension=0, tiled=True
        )

    sum_o = row_sum(grad_pack_o)
    sum_i = row_sum(grad_pack_i)
    grad_normed = token_sum(part)
    grad_more, grad_shift_b, grad_scale_b = modulate_grad(hidden_c, shift_b, scale_b, grad_normed)
    grad_hidden = grad_hidden + grad_more
    grad_branch = token_gather(grad_hidden.astype(bfloat))
    grad_mixed = (
        product(grad_branch, full_c[:, 3 * lw :])
        .astype(bfloat)
        .reshape(SLOTS, per_sample, head_count, HEAD_DIM)
    )
    grad_query, grad_key, grad_value = attend_backward(
        query_c, key_c, value_c, logsum_c, grad_mixed
    )
    grad_query = grad_query.astype(bfloat).reshape(TOK_DEV, lw)
    grad_kv = jnp.concatenate(
        [
            grad_key.astype(bfloat).reshape(SLOTS * CAP_LEN, lw),
            grad_value.astype(bfloat).reshape(SLOTS * CAP_LEN, lw),
        ],
        axis=1,
    )
    part = contract("te,de->td", grad_query, full_c[:, 0:lw])
    part_context = contract("re,de->rd", grad_kv, full_c[:, lw : 3 * lw])
    sum_c = row_sum(
        jnp.concatenate(
            [
                contract("td,te->de", hidden_low, grad_query),
                contract("rd,re->de", context_low, grad_kv),
                contract("td,te->de", grad_branch, mixed_c_low),
            ],
            axis=1,
        )
    )
    grad_hidden = grad_hidden + token_sum(part)
    grad_gate_a = jnp.sum(grad_hidden * branch_t, axis=0, keepdims=True)
    grad_branch = token_gather((gate_a * grad_hidden).astype(bfloat))
    grad_mixed = temporal_heads(
        product(grad_branch, full_t[:, 3 * lw :]).astype(bfloat), head_count
    )
    grads_t = attend_backward(*qkv_t, logsum_t, grad_mixed)
    grad_qkv = from_frames(jnp.stack(grads_t).astype(bfloat), head_count)
    grad_qkv = jnp.concatenate([grad_qkv[0], grad_qkv[1], grad_qkv[2]], axis=1)
    part = contract("te,de->td", grad_qkv, full_t[:, 0 : 3 * lw])
    sum_t = row_sum(
        jnp.concatenate(
            [
                contract("td,te->de", timed_low, grad_qkv),
                contract("td,te->de", grad_branch, mixed_t_low),
            ],
            axis=1,
        )
    )
    grad_hidden = grad_hidden + token_sum(part)
    grad_gate_a = grad_gate_a + jnp.sum(grad_hidden * branch_s, axis=0, keepdims=True)
    grad_branch = token_gather((gate_a * grad_hidden).astype(bfloat))
    grad_mixed = spatial_heads(
        product(grad_branch, full_s[:, 3 * lw :]).astype(bfloat), head_count
    )
    grads_s = attend_backward(*qkv_s, logsum_s, grad_mixed)
    grad_qkv = jnp.concatenate(
        [grad.astype(bfloat).reshape(TOK_DEV, lw) for grad in grads_s], axis=1
    )
    part = contract("te,de->td", grad_qkv, full_s[:, 0 : 3 * lw])
    sum_s = row_sum(
        jnp.concatenate(
            [
                contract("td,te->de", normed_a, grad_qkv),
                contract("td,te->de", grad_branch, mixed_s_low),
            ],
            axis=1,
        )
    )
    grad_context = cut_samples(
        token_gather(token_sum(pad_samples(part_context)).astype(bfloat))
    )
    grad_cap2 = contract("rd,re->de", grad_context, cap_act)
    grad_cap_mid = act_grad(
        gelu_tanh, cap_mid, contract("rd,de->re", grad_context, full_c2)
    ).astype(bfloat)
    grad_cap = contract("rc,re->ce", cap_rows, grad_cap_mid)
    sum_x = row_sum(
        jnp.concatenate(
            [
                grad_cap.reshape(dp_size, cap_rows_own, lw),
                grad_cap2.reshape(dp_size, row_count_own, lw),
            ],
            axis=1,
        ).reshape(dp_size * (cap_rows_own + row_count_own), lw)
    )
    grad_normed = token_sum(part)
    grad_more, grad_shift_a, grad_scale_a = modulate_grad(start_own, shift_a, scale_a, grad_normed)
    grad_hidden = grad_hidden + grad_more
    grad_patch = contract("ti,td->id", own_rows(patches), grad_hidden.astype(bfloat))
    grad_mods = jnp.concatenate(
        [
            grad_shift_a, grad_scale_a, grad_gate_a, grad_shift_b, grad_scale_b, grad_gate_b,
            grad_shift_f, grad_scale_f,
        ],
        axis=0,
    )
    placed = jnp.where(
        (jnp.arange(SLOTS) == sample)[:, None, None], grad_mods[None], 0.0
    )
    grad_mods = lax.psum(placed, "mp")
    mods_all = lax.all_gather(grad_mods.astype(bfloat), "dp", axis=0, tiled=True)
    grad_mods_low = mods_all[:, 0:6]
    grad_tables = jnp.sum(mods_all.astype(jnp.float32), axis=0)
    grad_temb_act = contract("ske,kde->sd", grad_mods_low, mod_rows)
    grad_temb = act_grad(jax.nn.silu, own_cols(time_emb_all), grad_temb_act) + own_cols(
        (mods_all[:, 6].astype(jnp.float32) + mods_all[:, 7].astype(jnp.float32))
    )
    grad_temb_low = lax.all_gather(grad_temb.astype(bfloat), "dp", axis=1, tiled=True)
    grad_first_own = act_grad(
        jax.nn.silu, own_cols(first_pre), contract("sd,id->si", grad_temb_low, temb_rows)
    ).astype(bfloat)
    grad_first = lax.all_gather(grad_first_own, "dp", axis=1, tiled=True)
    grad_time = contract("sd,ske->kde", own_cols(temb_act), grad_mods_low)
    grad_temb_part = contract("si,sd->id", own_cols(first_act), grad_temb_low)
    grad_freq = contract("sf,sd->fd", features, grad_first)
    small_part = lax.psum(jnp.concatenate([grad_patch, grad_final], axis=0), ("dp", "mp"))
    sum_small = jnp.concatenate([small_part[0:16], grad_freq, grad_tables, small_part[16:]], axis=0)

    def all_columns(rows):
        blocks = lax.all_gather(rows, "mp", axis=0, tiled=False)
        kinds = rows.shape[1] // lw
        stacked = blocks.reshape(mp_size, rows.shape[0], kinds, lw)
        return stacked.transpose(2, 1, 0, 3).reshape(kinds, rows.shape[0], mp_size * lw)

    whole_s, whole_t, whole_c, whole_i, whole_o, whole_x = [
        all_columns(rows).astype(jnp.float32)
        for rows in (sum_s, sum_t, sum_c, sum_i, sum_o, sum_x)
    ]
    sum_in = jnp.concatenate(
        [whole_s[0:3], whole_t[0:3], whole_c[0:3], whole_i, grad_time, grad_temb_part[None]], axis=0
    )
    sum_out = jnp.concatenate(
        [whole_s[3:4], whole_t[3:4], whole_c[3:4], whole_o, whole_x[:, cap_rows_own:]], axis=0
    )
    sum_cap = whole_x[0, 0:cap_rows_own]
    count_local = counts[0].astype(jnp.float32)
    square_in = sum_in * sum_in
    square_out = sum_out * sum_out
    square_cap = sum_cap * sum_cap
    square_small = sum_small * sum_small
    row_in_total = jnp.sum(square_in, axis=2)
    row_out_total = jnp.sum(square_out, axis=2)
    row_cap_total = jnp.sum(square_cap, axis=1)
    row_small_total = jnp.sum(square_small, axis=1)
    col_small_total = jnp.sum(square_small, axis=0)
    col_in_total, col_out_total, col_cap_total, loss_total, count_total = (
        lax.psum(jnp.sum(square_in, axis=1).astype(jnp.bfloat16), "dp").astype(jnp.float32),
        lax.psum(jnp.sum(square_out, axis=1).astype(jnp.bfloat16), "dp").astype(jnp.float32),
        lax.psum(jnp.sum(square_cap, axis=0).astype(jnp.bfloat16), "dp").astype(jnp.float32),
        lax.psum(loss_local, ("dp", "mp")),
        lax.psum(count_local, "dp"),
    )
    inverse = 1.0 / count_total
    inverse_sq = inverse * inverse
    rows_in_new = new_stat(rows_in, row_in_total, D, inverse_sq)
    cols_in_new = new_stat(cols_in, col_in_total, D, inverse_sq)
    rows_out_new = new_stat(rows_out, row_out_total, D, inverse_sq)
    cols_out_new = new_stat(cols_out, col_out_total, D, inverse_sq)
    rows_cap_new = new_stat(rows_cap, row_cap_total, D, inverse_sq)
    cols_cap_new = new_stat(cols_cap, col_cap_total, CAP_DIM, inverse_sq)
    rows_small_new = new_stat(rows_small, row_small_total, D, inverse_sq)
    cols_small_new = new_stat(cols_small, col_small_total, small_rows, inverse_sq)
    grad_in = sum_in * inverse
    grad_out = sum_out * inverse
    grad_cap_all = (sum_cap * inverse)[None]
    grad_small_all = (sum_small * inverse)[None]
    ratios = lax.psum(
        jnp.concatenate(
            [
                ratio_terms(w_in, grad_in, rows_in_new, cols_in_new),
                ratio_terms(w_out, grad_out, rows_out_new, cols_out_new),
                ratio_terms(w_cap[None], grad_cap_all, rows_cap_new[None], cols_cap_new[None]),
            ],
            axis=1,
        ),
        "dp",
    )
    totals = jnp.concatenate(
        [
            ratios,
            ratio_terms(w_small[None], grad_small_all, rows_small_new[None], cols_small_new[None]),
        ],
        axis=1,
    )
    row_count = jnp.array([float(D)] * 28 + [float(CAP_DIM), float(small_rows)], jnp.float32)
    mean_rows = totals[0] / row_count
    spreads = jnp.sqrt(mean_rows * totals[1] / (row_count * D))
    weight_scale = jnp.sqrt(totals[2] / (row_count * D))
    in_new, in_copy, in_update = apply_update(
        w_in, grad_in, rows_in_new, cols_in_new, mean_rows[0:20], spreads[0:20], weight_scale[0:20]
    )
    out_new, out_copy, out_update = apply_update(
        w_out,
        grad_out,
        rows_out_new,
        cols_out_new,
        mean_rows[20:28],
        spreads[20:28],
        weight_scale[20:28],
    )
    cap_new, cap_copy, cap_update = apply_update(
        w_cap[None],
        grad_cap_all,
        rows_cap_new[None],
        cols_cap_new[None],
        mean_rows[28:29],
        spreads[28:29],
        weight_scale[28:29],
    )
    small_new, small_copy, small_update = apply_update(
        w_small[None],
        grad_small_all,
        rows_small_new[None],
        cols_small_new[None],
        mean_rows[29:30],
        spreads[29:30],
        weight_scale[29:30],
    )
    return (
        loss_total * inverse,
        in_new,
        in_copy,
        in_update,
        rows_in_new,
        cols_in_new,
        out_new,
        out_copy,
        out_update,
        rows_out_new,
        cols_out_new,
        cap_new[0],
        cap_copy[0],
        cap_update[0],
        rows_cap_new,
        cols_cap_new,
        small_new[0],
        small_copy[0],
        small_update[0],
        rows_small_new,
        cols_small_new,
        spreads,
    )


def solution(mesh):
    in_specs = (
        P("dp", None, None, None),
        P("dp", None, None, None),
        P("dp"),
        P("dp"),
        P("dp", None, None),
        P(None, "dp", None),
        P(None, "dp", None),
        P("dp", None),
        P(),
        P(None, "dp"),
        P(),
        P(None, "dp"),
        P(),
        P("dp"),
        P(),
        P(),
        P(),
    )
    out_specs = (
        P(),
        P(None, "dp", None),
        P(None, "dp", None),
        P(None, "dp", None),
        P(None, "dp"),
        P(),
        P(None, "dp", None),
        P(None, "dp", None),
        P(None, "dp", None),
        P(None, "dp"),
        P(),
        P("dp", None),
        P("dp", None),
        P("dp", None),
        P("dp"),
        P(),
        P(),
        P(),
        P(),
        P(),
        P(),
        P(),
    )
    return jax.shard_map(shards, mesh=mesh, in_specs=in_specs, out_specs=out_specs, check_vma=False)
```

```python
import math

import jax
import jax.numpy as jnp
from jax import lax
from jax.experimental import pallas as pl
from jax.experimental.pallas import tpu as pltpu
from jax.sharding import PartitionSpec as P

HEAD_DIM = 72
D = 1152
FREQ = 256
CAP_DIM = 4096
CAP_LEN = 120
FRAMES = 8
GRID_H = 4
GRID_W = 8
PATCHES = 32
SLOTS = 2
STEP = 20
TOK_DEV = 512
CAP_PAD = 128


norm_eps = 1e-06
relative_rate = 0.5
tanh_coeff = math.sqrt(2.0 / math.pi)
angle_unit = math.pi / 2.0 / 1.008 / 1000.0


def product(left, right):
    return jnp.dot(left, right, preferred_element_type=jnp.float32)


def contract(form, left, right):
    return jnp.einsum(form, left, right, preferred_element_type=jnp.float32)


def gelu_tanh(values):
    return (
        0.5 * values * (1.0 + jnp.tanh(tanh_coeff * (values + 0.044715 * values * values * values)))
    )


def layer_norm(values):
    center = values - jnp.mean(values, axis=-1, keepdims=True)
    return center * lax.rsqrt(jnp.mean(center * center, axis=-1, keepdims=True) + norm_eps)


def modulate(hidden, shift_rows, scale_rows):
    return layer_norm(hidden) * (1.0 + scale_rows) + shift_rows


def modulate_grad(hidden, shift_rows, scale_rows, grad_rows):
    pullback = jax.vjp(modulate, hidden, shift_rows, scale_rows)[1]
    return pullback(grad_rows)


def act_grad(function, values, grad_rows):
    return jax.vjp(function, values)[1](grad_rows)[0]


def sincos(positions, table_width):
    half_width = table_width // 2
    frequency = jnp.exp(
        -math.log(10000.0) * jnp.arange(half_width).astype(jnp.float32) / half_width
    )
    angles = positions[:, None] * frequency[None, :]
    return jnp.concatenate([jnp.sin(angles), jnp.cos(angles)], axis=1)


def position_tables():
    patch_index = jnp.arange(GRID_H * GRID_W)
    spatial = jnp.concatenate(
        [
            sincos((patch_index // GRID_W).astype(jnp.float32), D // 2),
            sincos((patch_index % GRID_W).astype(jnp.float32), D // 2),
        ],
        axis=1,
    )
    temporal = sincos(jnp.arange(FRAMES).astype(jnp.float32), D)
    return (spatial, temporal)


def time_features(timesteps):
    half_width = FREQ // 2
    frequency = jnp.exp(
        -math.log(10000.0) * jnp.arange(half_width).astype(jnp.float32) / half_width
    )
    angles = timesteps.astype(jnp.float32)[:, None] * frequency[None, :]
    return jnp.concatenate([jnp.cos(angles), jnp.sin(angles)], axis=1)


def plan(timesteps):
    moment = timesteps.astype(jnp.float32)
    start_angle = 8.0 * angle_unit
    cos_start = math.cos(start_angle) ** 2
    remain_now = jnp.sin((1000.0 - moment) * angle_unit)
    remain_before = jnp.sin((1001.0 - moment) * angle_unit)
    alpha_now = remain_now * remain_now / cos_start
    alpha_before = remain_before * remain_before / cos_start
    rest_now = (
        jnp.sin(2.0 * start_angle + moment * angle_unit) * jnp.sin(moment * angle_unit) / cos_start
    )
    rest_before = (
        jnp.sin(2.0 * start_angle + (moment - 1.0) * angle_unit)
        * jnp.sin((moment - 1.0) * angle_unit)
        / cos_start
    )
    beta_now = (
        jnp.sin(2.0 * start_angle + (2.0 * moment - 1.0) * angle_unit)
        * math.sin(angle_unit)
        / (remain_before * remain_before)
    )
    posterior = beta_now * rest_before / rest_now
    kappa = beta_now * beta_now * alpha_before / (rest_now * alpha_now)
    return (alpha_now, rest_now, beta_now, posterior, kappa)


def patch_terms(output, target, squared, beta_rows, posterior_rows, kappa_rows):
    error_rows = output[:, :, 0:4] - target
    log_beta = jnp.log(beta_rows)[:, None, None]
    log_post = jnp.log(posterior_rows)[:, None, None]
    fraction = (output[:, :, 4:8] + 1.0) * 0.5
    log_model = fraction * log_beta + (1.0 - fraction) * log_post
    diverge = 0.5 * (
        -1.0
        + log_model
        - log_post
        + jnp.exp(log_post - log_model)
        + kappa_rows[:, None, None] * squared * jnp.exp(-log_model)
    )
    return jnp.mean(error_rows * error_rows, axis=(1, 2)) + jnp.mean(
        diverge, axis=(1, 2)
    ) / math.log(2.0)


def to_frames(stacked, head_count):
    leading = stacked.shape[0]
    return (
        stacked.reshape(leading, SLOTS, FRAMES, PATCHES, head_count, HEAD_DIM)
        .transpose(0, 1, 3, 2, 4, 5)
        .reshape(leading, SLOTS * PATCHES, FRAMES, head_count, HEAD_DIM)
    )


def from_frames(stacked, head_count):
    leading = stacked.shape[0]
    return (
        stacked.reshape(leading, SLOTS, PATCHES, FRAMES, head_count, HEAD_DIM)
        .transpose(0, 1, 3, 2, 4, 5)
        .reshape(leading, SLOTS * FRAMES * PATCHES, head_count * HEAD_DIM)
    )


def attend_forward(queries, key_rows, value_rows):
    scores = contract("bqhc,bkhc->bhqk", queries, key_rows) * HEAD_DIM ** (-0.5)
    highest = jnp.max(scores, axis=-1, keepdims=True)
    shifted = jnp.exp(scores - highest)
    denominator = jnp.sum(shifted, axis=-1, keepdims=True)
    weights = (shifted / denominator).astype(jnp.bfloat16)
    return (contract("bhqk,bkhc->bqhc", weights, value_rows), highest + jnp.log(denominator))


def attend_backward(queries, key_rows, value_rows, logsum, grad_mixed):
    scores = contract("bqhc,bkhc->bhqk", queries, key_rows) * HEAD_DIM ** (-0.5)
    probability = jnp.exp(scores - logsum)
    grad_value = contract("bhqk,bqhc->bkhc", probability.astype(jnp.bfloat16), grad_mixed)
    grad_prob = contract("bqhc,bkhc->bhqk", grad_mixed, value_rows)
    grad_scores = (
        probability * (grad_prob - jnp.sum(probability * grad_prob, axis=-1, keepdims=True))
    ).astype(jnp.bfloat16)
    grad_query = contract("bhqk,bkhc->bqhc", grad_scores, key_rows) * HEAD_DIM ** (-0.5)
    grad_key = contract("bhqk,bqhc->bkhc", grad_scores, queries) * HEAD_DIM ** (-0.5)
    return (grad_query, grad_key, grad_value)


def new_stat(old_stat, sums, length, inverse_sq):
    rho = 1.0 - STEP ** (-0.8)
    return rho * old_stat + (1.0 - rho) * (sums * inverse_sq / length + 1e-30)


def ratio_terms(weight, grad, rows_new, cols_new):
    ratio = jnp.sum(grad * grad / (rows_new[:, :, None] * cols_new[:, None, :]), axis=(1, 2))
    return jnp.stack([jnp.sum(rows_new, axis=1), ratio, jnp.sum(weight * weight, axis=(1, 2))])


def apply_update(weight, grad, rows_new, cols_new, mean_rows, spread, weight_scale):
    second = rows_new[:, :, None] * cols_new[:, None, :] / mean_rows[:, None, None]
    update = grad * lax.rsqrt(second)
    clipped = update / jnp.maximum(1.0, spread)[:, None, None]
    new_weight = weight - relative_rate * weight_scale[:, None, None] * clipped
    return (new_weight, new_weight.astype(jnp.bfloat16), clipped)


MESH_ID = pl.DeviceIdType.MESH
ROW_STEP = 16


def remote(source, target, send_sem, recv_sem, device):
    return pltpu.make_async_remote_copy(
        src_ref=source,
        dst_ref=target,
        send_sem=send_sem,
        recv_sem=recv_sem,
        device_id=device,
        device_id_type=MESH_ID,
    )


def greet(devices):
    barrier = pltpu.get_barrier_semaphore()
    for device in devices:
        pl.semaphore_signal(barrier, inc=1, device_id=device, device_id_type=MESH_ID)
    pl.semaphore_wait(barrier, len(devices))


def exchange(axis, arrays, shared, number):
    size = lax.axis_size(axis)
    count = len(arrays)

    def kernel(*refs):
        sources, results = refs[0:count], refs[count : 2 * count]
        send_sem, recv_sem = refs[2 * count :]
        me = lax.axis_index(axis)
        peers = [lax.rem(me + step, size) for step in range(1, size)]
        greet([{axis: peer} for peer in peers])
        copies = []
        for step, peer in enumerate(peers):
            for at in range(count):
                source = sources[at] if shared[at] else sources[at].at[peer]
                copy = remote(
                    source,
                    results[at].at[me],
                    send_sem.at[at, step],
                    recv_sem.at[at, step],
                    {axis: peer},
                )
                copy.start()
                copies.append(copy)
        for at in range(count):
            own = sources[at][...] if shared[at] else sources[at][me]
            results[at][me] = own
        for copy in copies:
            copy.wait()

    shapes = [
        jax.ShapeDtypeStruct((size,) + (array.shape if keep else array.shape[1:]), array.dtype)
        for array, keep in zip(arrays, shared)
    ]
    vmem = pl.BlockSpec(memory_space=pltpu.VMEM)
    return pl.pallas_call(
        kernel,
        out_shape=shapes,
        in_specs=[vmem] * count,
        out_specs=[vmem] * count,
        scratch_shapes=[
            pltpu.SemaphoreType.DMA((count, size - 1)),
            pltpu.SemaphoreType.DMA((count, size - 1)),
        ],
        compiler_params=pltpu.CompilerParams(collective_id=number, has_side_effects=True),
        name=f"exchange_{axis}_{number}",
    )(*arrays)


def across(pieces, own, step_rows, row_types, sums, gather, number):
    size = lax.axis_size("mp")
    chips = size // 2
    adds = pieces is not None
    rows = pieces.shape[0] // size if adds else own[0].shape[0]
    width = own[0].shape[1] if own else pieces.shape[1]
    bfloat = jnp.bfloat16
    n_own, n_rows = len(own), len(row_types)

    def kernel(*refs):
        refs = list(refs)
        if adds:
            part = refs.pop(0)
        owns, refs = refs[0:n_own], refs[n_own:]
        row_refs, refs = refs[0:n_rows], refs[n_rows:]
        sum_refs, refs = refs[0:sums], refs[sums:]
        if gather:
            full = refs.pop(0)
        if adds:
            near, away, far, near_send, near_recv, far_send, far_recv = refs[0:7]
            refs = refs[7:]
        me = lax.axis_index("mp")
        core = lax.rem(me, 2)
        chip = me // 2
        partner = me + 1 - 2 * core

        def device(number_at):
            return {"mp": number_at}

        def at_step(step):
            return lax.rem(chip + step, chips)

        def block(number_at):
            return pl.ds(pl.multiple_of(number_at * rows, rows), rows)

        greet([device(partner)] + [device(at_step(k) * 2 + core) for k in range(1, chips)])
        pending = []
        if adds:
            near_copies = {}
            for k in list(range(1, chips)) + [0]:
                copy = remote(
                    part.at[block(at_step(k) * 2 + 1 - core)],
                    near.at[k],
                    near_send.at[k],
                    near_recv.at[k],
                    device(partner),
                )
                copy.start()
                near_copies[k] = copy
                pending.append(copy)
            far_copies = []
            for k in range(1, chips):
                near_copies[k].wait_recv()
                start = (at_step(k) * 2 + core) * rows

                @pl.loop(0, rows // ROW_STEP)
                def _(i):
                    here = pl.ds(pl.multiple_of(i * ROW_STEP, ROW_STEP), ROW_STEP)
                    there = pl.ds(pl.multiple_of(start + i * ROW_STEP, ROW_STEP), ROW_STEP)
                    away[k - 1, here] = (
                        part[there].astype(jnp.float32) + near[k, here].astype(jnp.float32)
                    ).astype(bfloat)

                copy = remote(
                    away.at[k - 1],
                    far.at[k - 1],
                    far_send.at[k - 1],
                    far_recv.at[k - 1],
                    device(at_step(k) * 2 + core),
                )
                copy.start()
                far_copies.append(copy)
                pending.append(copy)
            near_copies[0].wait_recv()
            for copy in far_copies:
                copy.wait_recv()
        for ref in sum_refs:
            ref[...] = jnp.zeros_like(ref)
        mine = me * rows

        @pl.loop(0, rows // ROW_STEP)
        def _(i):
            here = pl.ds(pl.multiple_of(i * ROW_STEP, ROW_STEP), ROW_STEP)
            there = pl.ds(pl.multiple_of(mine + i * ROW_STEP, ROW_STEP), ROW_STEP)
            values = [ref[here] if ref.shape[0] == rows else ref[...] for ref in owns]
            if adds:
                total = part[there].astype(jnp.float32) + near[0, here].astype(jnp.float32)
                for k in range(1, chips):
                    total = total + far[k - 1, here].astype(jnp.float32)
                row_values, terms, sent = step_rows(total, *values)
            else:
                row_values, terms, sent = [], [], values[0]
            for ref, value in zip(row_refs, row_values):
                ref[here] = value.astype(ref.dtype)
            for ref, value in zip(sum_refs, terms):
                ref[...] += jnp.sum(value.reshape(ROW_STEP // 8, 8, width), axis=0)
            if gather:
                full[there] = sent.astype(bfloat)

        if gather:
            out_send, out_recv, back_send, back_recv = refs
            outward = []
            for k in list(range(1, chips)) + [0]:
                copy = remote(
                    full.at[block(me)],
                    full.at[block(me)],
                    out_send.at[k],
                    out_recv.at[k],
                    device(at_step(k) * 2 + core) if k else device(partner),
                )
                copy.start()
                outward.append(copy)
                pending.append(copy)
            backward = []
            for k in range(1, chips):
                outward[k - 1].wait_recv()
                came = at_step(chips - k) * 2 + core
                copy = remote(
                    full.at[block(came)],
                    full.at[block(came)],
                    back_send.at[k - 1],
                    back_recv.at[k - 1],
                    device(partner),
                )
                copy.start()
                backward.append(copy)
                pending.append(copy)
            outward[-1].wait_recv()
            for copy in backward:
                copy.wait_recv()
        for copy in pending:
            copy.wait_send()

    dma = pltpu.SemaphoreType.DMA
    shapes = [jax.ShapeDtypeStruct((rows, width), kind) for kind in row_types]
    shapes += [jax.ShapeDtypeStruct((8, width), jnp.float32)] * sums
    scratch = []
    if gather:
        shapes.append(jax.ShapeDtypeStruct((rows * size, width), bfloat))
    if adds:
        scratch += [
            pltpu.VMEM((chips, rows, width), bfloat),
            pltpu.VMEM((chips - 1, rows, width), bfloat),
            pltpu.VMEM((chips - 1, rows, width), bfloat),
            dma((chips,)),
            dma((chips,)),
            dma((chips - 1,)),
            dma((chips - 1,)),
        ]
    if gather:
        scratch += [dma((chips,)), dma((chips,)), dma((chips - 1,)), dma((chips - 1,))]
    vmem = pl.BlockSpec(memory_space=pltpu.VMEM)
    inputs = ([pieces] if adds else []) + list(own)
    return pl.pallas_call(
        kernel,
        out_shape=shapes,
        in_specs=[vmem] * len(inputs),
        out_specs=[vmem] * len(shapes),
        scratch_shapes=scratch,
        compiler_params=pltpu.CompilerParams(collective_id=number, has_side_effects=True),
        name=f"across_{number}",
    )(*inputs)


def normalize(values):
    center = values - jnp.mean(values, axis=-1, keepdims=True)
    spread = lax.rsqrt(jnp.mean(center * center, axis=-1, keepdims=True) + norm_eps)
    return center * spread, spread


def normalize_grad(normal, spread, grad_rows):
    mean_grad = jnp.mean(grad_rows, axis=-1, keepdims=True)
    mean_both = jnp.mean(grad_rows * normal, axis=-1, keepdims=True)
    return spread * (grad_rows - mean_grad - normal * mean_both)


def pad_samples(rows):
    stacked = rows.reshape(SLOTS, CAP_LEN, rows.shape[1])
    padded = jnp.pad(stacked, ((0, 0), (0, CAP_PAD - CAP_LEN), (0, 0)))
    return padded.reshape(SLOTS * CAP_PAD, rows.shape[1])


def cut_samples(rows):
    stacked = rows.reshape(SLOTS, CAP_PAD, rows.shape[1])[:, 0:CAP_LEN]
    return stacked.reshape(SLOTS * CAP_LEN, rows.shape[1])


def side_by_side(stacked):
    return stacked.transpose(1, 0, 2).reshape(stacked.shape[1], -1)


def heads_of(rows, lead, count):
    return rows.reshape(*lead, count, HEAD_DIM)


def spatial_heads(rows, count):
    return rows.reshape(SLOTS * FRAMES, PATCHES, count, HEAD_DIM)


def temporal_heads(rows, count):
    return to_frames(rows[None], count)[0]


def shards(
    latents, gaussian_noise, timesteps, counts, captions,
    w_in, w_out, w_cap, w_small,
    rows_in, cols_in, rows_out, cols_out, rows_cap, cols_cap, rows_small, cols_small,
):
    bfloat = jnp.bfloat16
    mp_index = lax.axis_index("mp")
    dp_index = lax.axis_index("dp")
    mp_size = lax.axis_size("mp")
    dp_size = lax.axis_size("dp")
    local_width = w_in.shape[2] // mp_size
    head_count = local_width // HEAD_DIM
    col_start = mp_index * local_width
    row_count_own = w_in.shape[1]
    row_start = dp_index * row_count_own
    cap_rows_own = w_cap.shape[0]
    small_rows = 56 + FREQ
    per_sample = FRAMES * PATCHES
    own_tokens = TOK_DEV // mp_size
    token_start = mp_index * own_tokens
    sample = token_start // per_sample
    wide = 4 * local_width
    lw = local_width

    in_cols = lax.dynamic_slice_in_dim(w_in[0:13], col_start, lw, 2).astype(bfloat)
    out_cols = lax.dynamic_slice_in_dim(w_out, col_start, lw, 2).astype(bfloat)
    cap_cols = lax.dynamic_slice_in_dim(w_cap, col_start, lw, 1).astype(bfloat)
    pack_s = side_by_side(jnp.concatenate([in_cols[0:3], out_cols[0:1]], axis=0))
    pack_t = side_by_side(jnp.concatenate([in_cols[3:6], out_cols[1:2]], axis=0))
    pack_c = side_by_side(jnp.concatenate([in_cols[6:9], out_cols[2:3]], axis=0))
    pack_i = side_by_side(in_cols[9:13])
    pack_o = side_by_side(out_cols[3:7])
    pack_x = jnp.concatenate([cap_cols, out_cols[7]], axis=0)
    full_s = lax.all_gather(pack_s, "dp", axis=0, tiled=True)
    full_t = lax.all_gather(pack_t, "dp", axis=0, tiled=True)
    full_x = lax.all_gather(pack_x, "dp", axis=0, tiled=False)
    full_c = lax.all_gather(pack_c, "dp", axis=0, tiled=True)
    full_i = lax.all_gather(pack_i, "dp", axis=0, tiled=True)
    full_o = lax.all_gather(pack_o, "dp", axis=0, tiled=True)
    full_cap = full_x[:, 0:cap_rows_own].reshape(CAP_DIM, lw)
    full_c2 = full_x[:, cap_rows_own:].reshape(D, lw)
    mod_rows = w_in[13:19].astype(bfloat)
    temb_rows = w_in[19].astype(bfloat)

    full_small = w_small.astype(bfloat)
    patch_w = full_small[0:16]
    freq_w = full_small[16 : 16 + FREQ]
    tables = full_small[16 + FREQ : 24 + FREQ].astype(jnp.float32)
    final_w = full_small[24 + FREQ :]

    def own_rows(rows):
        return lax.dynamic_slice_in_dim(rows, token_start, own_tokens, 0)

    def own_cols(rows):
        return lax.dynamic_slice_in_dim(rows, row_start, row_count_own, 1)

    numbers = jnp.zeros((8, 128), jnp.int32)
    numbers = numbers.at[0, 0:SLOTS].set(timesteps).at[0, SLOTS].set(counts[0])
    numbers_all = exchange("dp", [numbers], [True], 1)[0]
    all_times = numbers_all[:, 0, 0:SLOTS].reshape(-1)
    count_total = jnp.sum(numbers_all[:, 0, SLOTS]).astype(jnp.float32)
    alpha_now, rest_now, beta_now, posterior, kappa = plan(timesteps)
    features = time_features(all_times).astype(bfloat)
    first_pre = product(features, freq_w)
    first_act = jax.nn.silu(first_pre).astype(bfloat)
    temb_part = product(own_cols(first_act), temb_rows)
    sample_count = temb_part.shape[0]
    temb_cols_all, temb_rows_all = exchange(
        "dp",
        [
            temb_part.reshape(sample_count, dp_size, row_count_own).transpose(1, 0, 2),
            temb_part.reshape(dp_size, SLOTS, D),
        ],
        [False, False],
        2,
    )
    time_cols = jnp.sum(temb_cols_all, axis=0)
    time_emb = jnp.sum(temb_rows_all, axis=0)
    temb_act = jax.nn.silu(time_cols).astype(bfloat)
    mod_part = contract("sd,kde->ske", temb_act, mod_rows)
    modulation = (
        jnp.sum(exchange("dp", [mod_part.reshape(dp_size, SLOTS * 6, D)], [False], 3)[0], axis=0)
        .reshape(SLOTS, 6, D)
        + tables[None, 0:6]
    )
    mods_own = lax.dynamic_index_in_dim(modulation, sample, 0, keepdims=False)
    shift_a, scale_a, gate_a, shift_b, scale_b, gate_b = [
        mods_own[number : number + 1] for number in range(6)
    ]
    temb_own = lax.dynamic_slice_in_dim(time_emb, sample, 1, 0)

    noisy_low = (
        jnp.sqrt(alpha_now)[:, None, None, None] * latents.astype(jnp.float32)
        + jnp.sqrt(rest_now)[:, None, None, None] * gaussian_noise
    ).astype(bfloat)
    patches = noisy_low.reshape(TOK_DEV, 16)
    spatial_pos, temporal_pos = position_tables()
    start_hidden = (
        product(patches, patch_w).reshape(SLOTS * FRAMES, PATCHES, D) + spatial_pos[None]
    ).reshape(SLOTS, per_sample, D)
    start_own = own_rows(start_hidden.reshape(TOK_DEV, D))

    cap_rows = captions.reshape(SLOTS * CAP_LEN, CAP_DIM)
    cap_mid = product(cap_rows, full_cap)
    cap_act = gelu_tanh(cap_mid).astype(bfloat)
    context_part = pad_samples(contract("re,de->rd", cap_act, full_c2).astype(bfloat))
    context_low = cut_samples(
        across(context_part, [], lambda total: ([], [], total), [], 0, True, 4)[0]
    )

    normed_a = (
        modulate(start_hidden, modulation[:, 0][:, None], modulation[:, 1][:, None])
        .astype(bfloat)
        .reshape(TOK_DEV, D)
    )
    qkv = product(normed_a, full_s[:, 0 : 3 * lw]).astype(bfloat)
    qkv_s = [spatial_heads(qkv[:, k * lw : (k + 1) * lw], head_count) for k in range(3)]
    mixed_s, logsum_s = attend_forward(*qkv_s)
    mixed_s_low = mixed_s.astype(bfloat).reshape(TOK_DEV, lw)
    frame_start = (token_start % per_sample) // PATCHES
    frames_own = own_tokens // PATCHES
    temporal_own = lax.dynamic_slice_in_dim(temporal_pos, frame_start, frames_own, 0)
    temporal_rows = jnp.broadcast_to(
        temporal_own[:, None, :], (frames_own, PATCHES, D)
    ).reshape(own_tokens, D)

    def spatial_step(total, start_rows, gate, position):
        hidden = start_rows + gate * total
        return [total, hidden], [], hidden + position

    f32 = jnp.float32
    branch_s, hidden_s, timed_low = across(
        contract("te,de->td", mixed_s_low, full_s[:, 3 * lw :]).astype(bfloat),
        [start_own, gate_a, temporal_rows],
        spatial_step,
        [f32, f32],
        0,
        True,
        5,
    )
    qkv = product(timed_low, full_t[:, 0 : 3 * lw]).astype(bfloat)
    qkv_t = [temporal_heads(qkv[:, k * lw : (k + 1) * lw], head_count) for k in range(3)]
    mixed_t, logsum_t = attend_forward(*qkv_t)
    mixed_t_low = from_frames(mixed_t.astype(bfloat)[None], head_count)[0]

    def temporal_step(total, hidden_rows, gate):
        hidden = hidden_rows + gate * total
        return [total, hidden], [], hidden

    branch_t, hidden_t, hidden_low = across(
        contract("te,de->td", mixed_t_low, full_t[:, 3 * lw :]).astype(bfloat),
        [hidden_s, gate_a],
        temporal_step,
        [f32, f32],
        0,
        True,
        6,
    )
    query_c = (
        product(hidden_low, full_c[:, 0:lw])
        .astype(bfloat)
        .reshape(SLOTS, per_sample, head_count, HEAD_DIM)
    )
    key_value = product(context_low, full_c[:, lw : 3 * lw]).astype(bfloat)
    key_c = key_value[:, 0:lw].reshape(SLOTS, CAP_LEN, head_count, HEAD_DIM)
    value_c = key_value[:, lw:].reshape(SLOTS, CAP_LEN, head_count, HEAD_DIM)
    mixed_c, logsum_c = attend_forward(query_c, key_c, value_c)
    mixed_c_low = mixed_c.astype(bfloat).reshape(TOK_DEV, lw)

    def cross_step(total, hidden_rows, shift, scale):
        hidden = hidden_rows + total
        return [hidden], [], normalize(hidden)[0] * (1.0 + scale) + shift

    hidden_c, normed_b = across(
        contract("te,de->td", mixed_c_low, full_c[:, 3 * lw :]).astype(bfloat),
        [hidden_t, shift_b, scale_b],
        cross_step,
        [f32],
        0,
        True,
        7,
    )
    inner_pre = product(normed_b, full_i)
    inner_act = gelu_tanh(inner_pre).astype(bfloat)
    shift_f = tables[6:7] + temb_own
    scale_f = tables[7:8] + temb_own

    def forward_step(total, hidden_rows, gate, shift, scale):
        hidden = hidden_rows + gate * total
        return [total, hidden, normalize(hidden)[0] * (1.0 + scale) + shift], [], None

    branch_m, hidden_m, normed_f = across(
        contract("te,de->td", inner_act, full_o).astype(bfloat),
        [hidden_c, gate_b, shift_f, scale_f],
        forward_step,
        [f32, f32, bfloat],
        0,
        False,
        8,
    )
    output = contract("td,od->to", normed_f, final_w).reshape(own_tokens, 4, 8)
    target = own_rows(gaussian_noise.reshape(TOK_DEV, 4, 4))
    error_rows = output[:, :, 0:4] - target
    squared = error_rows * error_rows
    live = (sample * per_sample < counts[0]).astype(jnp.float32)

    def of_sample(values):
        return jnp.broadcast_to(lax.dynamic_slice_in_dim(values, sample, 1, 0), (own_tokens,))

    beta_rows = of_sample(beta_now)
    posterior_rows = of_sample(posterior)
    kappa_rows = of_sample(kappa)

    def patch_loss(values):
        return jnp.sum(
            patch_terms(values, target, squared, beta_rows, posterior_rows, kappa_rows) * live
        )

    loss_local, loss_pull = jax.vjp(patch_loss, output)
    grad_output = loss_pull(jnp.ones_like(loss_local))[0].astype(bfloat).reshape(own_tokens, 32)
    grad_final = contract("to,td->od", grad_output, normed_f)
    grad_normed = contract("to,od->td", grad_output, final_w)
    grad_hidden, grad_shift_f, grad_scale_f = modulate_grad(hidden_m, shift_f, scale_f, grad_normed)
    grad_gate_b = jnp.sum(grad_hidden * branch_m, axis=0, keepdims=True)
    grad_branch = across(
        None, [(gate_b * grad_hidden).astype(bfloat)], None, [], 0, True, 9
    )[0]
    grad_inner = act_grad(gelu_tanh, inner_pre, product(grad_branch, full_o)).astype(bfloat)
    part = contract("te,de->td", grad_inner, full_i)
    grad_pack_o = contract("td,te->de", grad_branch, inner_act)
    grad_pack_i = contract("td,te->de", normed_b, grad_inner)

    def row_sum(pieces):
        return lax.psum_scatter(
            pieces.astype(bfloat), "dp", scatter_dimension=0, tiled=True
        )

    sum_o = row_sum(grad_pack_o)
    sum_i = row_sum(grad_pack_i)

    def forward_grad_step(total, hidden_rows, scale, grad_rows):
        normal, spread = normalize(hidden_rows)
        grad = grad_rows + normalize_grad(normal, spread, total * (1.0 + scale))
        return [grad], [total, total * normal], grad

    def one_row(rows):
        return jnp.sum(rows, axis=0, keepdims=True)

    grad_hidden, grad_shift_b, grad_scale_b, grad_branch = across(
        part.astype(bfloat),
        [hidden_c, scale_b, grad_hidden],
        forward_grad_step,
        [f32],
        2,
        True,
        10,
    )
    grad_mixed = (
        product(grad_branch, full_c[:, 3 * lw :])
        .astype(bfloat)
        .reshape(SLOTS, per_sample, head_count, HEAD_DIM)
    )
    grad_query, grad_key, grad_value = attend_backward(
        query_c, key_c, value_c, logsum_c, grad_mixed
    )
    grad_query = grad_query.astype(bfloat).reshape(TOK_DEV, lw)
    grad_kv = jnp.concatenate(
        [
            grad_key.astype(bfloat).reshape(SLOTS * CAP_LEN, lw),
            grad_value.astype(bfloat).reshape(SLOTS * CAP_LEN, lw),
        ],
        axis=1,
    )
    part = contract("te,de->td", grad_query, full_c[:, 0:lw])
    part_context = contract("re,de->rd", grad_kv, full_c[:, lw : 3 * lw])
    sum_c = row_sum(
        jnp.concatenate(
            [
                contract("td,te->de", hidden_low, grad_query),
                contract("rd,re->de", context_low, grad_kv),
                contract("td,te->de", grad_branch, mixed_c_low),
            ],
            axis=1,
        )
    )

    def gated_step(total, grad_rows, branch_rows, gate):
        grad = grad_rows + total
        return [grad], [grad * branch_rows], gate * grad

    grad_hidden, grad_gate_t, grad_branch = across(
        part.astype(bfloat), [grad_hidden, branch_t, gate_a], gated_step, [f32], 1, True, 11
    )
    grad_mixed = temporal_heads(
        product(grad_branch, full_t[:, 3 * lw :]).astype(bfloat), head_count
    )
    grads_t = attend_backward(*qkv_t, logsum_t, grad_mixed)
    grad_qkv = from_frames(jnp.stack(grads_t).astype(bfloat), head_count)
    grad_qkv = jnp.concatenate([grad_qkv[0], grad_qkv[1], grad_qkv[2]], axis=1)
    part = contract("te,de->td", grad_qkv, full_t[:, 0 : 3 * lw])
    sum_t = row_sum(
        jnp.concatenate(
            [
                contract("td,te->de", timed_low, grad_qkv),
                contract("td,te->de", grad_branch, mixed_t_low),
            ],
            axis=1,
        )
    )
    grad_hidden, grad_gate_s, grad_branch = across(
        part.astype(bfloat), [grad_hidden, branch_s, gate_a], gated_step, [f32], 1, True, 12
    )
    grad_mixed = spatial_heads(
        product(grad_branch, full_s[:, 3 * lw :]).astype(bfloat), head_count
    )
    grads_s = attend_backward(*qkv_s, logsum_s, grad_mixed)
    grad_qkv = jnp.concatenate(
        [grad.astype(bfloat).reshape(TOK_DEV, lw) for grad in grads_s], axis=1
    )
    part = contract("te,de->td", grad_qkv, full_s[:, 0 : 3 * lw])
    sum_s = row_sum(
        jnp.concatenate(
            [
                contract("td,te->de", normed_a, grad_qkv),
                contract("td,te->de", grad_branch, mixed_s_low),
            ],
            axis=1,
        )
    )
    grad_context = cut_samples(
        across(
            pad_samples(part_context.astype(bfloat)),
            [],
            lambda total: ([], [], total),
            [],
            0,
            True,
            13,
        )[0]
    )
    grad_cap2 = contract("rd,re->de", grad_context, cap_act)
    grad_cap_mid = act_grad(
        gelu_tanh, cap_mid, contract("rd,de->re", grad_context, full_c2)
    ).astype(bfloat)
    grad_cap = contract("rc,re->ce", cap_rows, grad_cap_mid)
    sum_x = row_sum(
        jnp.concatenate(
            [
                grad_cap.reshape(dp_size, cap_rows_own, lw),
                grad_cap2.reshape(dp_size, row_count_own, lw),
            ],
            axis=1,
        ).reshape(dp_size * (cap_rows_own + row_count_own), lw)
    )

    def start_grad_step(total, hidden_rows, scale, grad_rows):
        normal, spread = normalize(hidden_rows)
        grad = grad_rows + normalize_grad(normal, spread, total * (1.0 + scale))
        return [grad], [total, total * normal], None

    grad_start, grad_shift_a, grad_scale_a = across(
        part.astype(bfloat),
        [start_own, scale_a, grad_hidden],
        start_grad_step,
        [bfloat],
        2,
        False,
        14,
    )
    grad_patch = contract("ti,td->id", own_rows(patches), grad_start)
    grad_mods = jnp.concatenate(
        [
            one_row(grad_shift_a), one_row(grad_scale_a), one_row(grad_gate_t + grad_gate_s),
            one_row(grad_shift_b), one_row(grad_scale_b), grad_gate_b,
            grad_shift_f, grad_scale_f,
        ],
        axis=0,
    )
    placed = jnp.where(
        (jnp.arange(SLOTS) == sample)[:, None, None], grad_mods[None], 0.0
    ).reshape(SLOTS * 8, D)
    small_rows_part = jnp.concatenate([grad_patch, grad_final], axis=0)
    small_count = small_rows_part.shape[0] // mp_size
    loss_block = jnp.broadcast_to(loss_local, (8, 128))
    placed_all, small_all, loss_all = exchange(
        "mp",
        [placed, small_rows_part.reshape(mp_size, small_count, D), loss_block],
        [True, False, True],
        15,
    )
    grad_mods = jnp.sum(placed_all, axis=0).reshape(SLOTS, 8, D)
    small_own = jnp.sum(small_all, axis=0).astype(bfloat)
    loss_part = jnp.sum(loss_all[:, 0, 0])
    mods_all, small_all = exchange(
        "dp", [grad_mods.astype(bfloat).reshape(SLOTS * 8, D), small_own], [True, True], 16
    )
    mods_all = mods_all.reshape(dp_size * SLOTS, 8, D)
    small_own = jnp.sum(small_all.astype(f32), axis=0)
    grad_mods_low = mods_all[:, 0:6]
    grad_tables = jnp.sum(mods_all.astype(f32), axis=0)
    grad_temb_act = contract("ske,kde->sd", grad_mods_low, mod_rows)
    grad_temb = act_grad(jax.nn.silu, time_cols, grad_temb_act) + own_cols(
        (mods_all[:, 6].astype(f32) + mods_all[:, 7].astype(f32))
    )

    def dp_columns(rows, number):
        blocks = exchange("dp", [rows], [True], number)[0]
        return blocks.transpose(1, 0, 2).reshape(rows.shape[0], D)

    grad_temb_low = dp_columns(grad_temb.astype(bfloat), 17)
    grad_first_own = act_grad(
        jax.nn.silu, own_cols(first_pre), contract("sd,id->si", grad_temb_low, temb_rows)
    ).astype(bfloat)
    grad_first = dp_columns(grad_first_own, 18)
    grad_time = contract("sd,ske->kde", temb_act, grad_mods_low)
    grad_temb_part = contract("si,sd->id", own_cols(first_act), grad_temb_low)
    grad_freq = contract("sf,sd->fd", features, grad_first)
    small_part = exchange("mp", [small_own], [True], 19)[0].reshape(mp_size * small_count, D)
    sum_small = jnp.concatenate([small_part[0:16], grad_freq, grad_tables, small_part[16:]], axis=0)

    def all_columns(rows):
        blocks = lax.all_gather(rows, "mp", axis=0, tiled=False)
        kinds = rows.shape[1] // lw
        stacked = blocks.reshape(mp_size, rows.shape[0], kinds, lw)
        return stacked.transpose(2, 1, 0, 3).reshape(kinds, rows.shape[0], mp_size * lw)

    whole_s, whole_t, whole_c, whole_i, whole_o, whole_x = [
        all_columns(rows).astype(jnp.float32)
        for rows in (sum_s, sum_t, sum_c, sum_i, sum_o, sum_x)
    ]
    sum_in = jnp.concatenate(
        [whole_s[0:3], whole_t[0:3], whole_c[0:3], whole_i, grad_time, grad_temb_part[None]], axis=0
    )
    sum_out = jnp.concatenate(
        [whole_s[3:4], whole_t[3:4], whole_c[3:4], whole_o, whole_x[:, cap_rows_own:]], axis=0
    )
    sum_cap = whole_x[0, 0:cap_rows_own]
    square_in = sum_in * sum_in
    square_out = sum_out * sum_out
    square_cap = sum_cap * sum_cap
    square_small = sum_small * sum_small
    row_in_total = jnp.sum(square_in, axis=2)
    row_out_total = jnp.sum(square_out, axis=2)
    row_cap_total = jnp.sum(square_cap, axis=1)
    row_small_total = jnp.sum(square_small, axis=1)
    col_small_total = jnp.sum(square_small, axis=0)
    col_part = jnp.concatenate(
        [
            jnp.sum(square_in, axis=1),
            jnp.sum(square_out, axis=1),
            jnp.sum(square_cap, axis=0, keepdims=True),
        ],
        axis=0,
    )
    col_all = exchange("dp", [col_part.astype(bfloat)], [True], 20)[0]
    col_total = jnp.sum(col_all.astype(f32), axis=0)
    col_in_total, col_out_total, col_cap_total = col_total[0:20], col_total[20:28], col_total[28]
    inverse = 1.0 / count_total
    inverse_sq = inverse * inverse
    rows_in_new = new_stat(rows_in, row_in_total, D, inverse_sq)
    cols_in_new = new_stat(cols_in, col_in_total, D, inverse_sq)
    rows_out_new = new_stat(rows_out, row_out_total, D, inverse_sq)
    cols_out_new = new_stat(cols_out, col_out_total, D, inverse_sq)
    rows_cap_new = new_stat(rows_cap, row_cap_total, D, inverse_sq)
    cols_cap_new = new_stat(cols_cap, col_cap_total, CAP_DIM, inverse_sq)
    rows_small_new = new_stat(rows_small, row_small_total, D, inverse_sq)
    cols_small_new = new_stat(cols_small, col_small_total, small_rows, inverse_sq)
    grad_in = sum_in * inverse
    grad_out = sum_out * inverse
    grad_cap_all = (sum_cap * inverse)[None]
    grad_small_all = (sum_small * inverse)[None]
    ratio_part = jnp.concatenate(
        [
            ratio_terms(w_in, grad_in, rows_in_new, cols_in_new),
            ratio_terms(w_out, grad_out, rows_out_new, cols_out_new),
            ratio_terms(w_cap[None], grad_cap_all, rows_cap_new[None], cols_cap_new[None]),
        ],
        axis=1,
    )
    ratio_block = jnp.zeros((8, 128), f32).at[0:3, 0:29].set(ratio_part).at[3, 0].set(loss_part)
    ratio_block = jnp.sum(exchange("dp", [ratio_block], [True], 21)[0], axis=0)
    ratios = ratio_block[0:3, 0:29]
    loss_total = ratio_block[3, 0]
    totals = jnp.concatenate(
        [
            ratios,
            ratio_terms(w_small[None], grad_small_all, rows_small_new[None], cols_small_new[None]),
        ],
        axis=1,
    )
    row_count = jnp.array([float(D)] * 28 + [float(CAP_DIM), float(small_rows)], jnp.float32)
    mean_rows = totals[0] / row_count
    spreads = jnp.sqrt(mean_rows * totals[1] / (row_count * D))
    weight_scale = jnp.sqrt(totals[2] / (row_count * D))
    in_new, in_copy, in_update = apply_update(
        w_in, grad_in, rows_in_new, cols_in_new, mean_rows[0:20], spreads[0:20], weight_scale[0:20]
    )
    out_new, out_copy, out_update = apply_update(
        w_out,
        grad_out,
        rows_out_new,
        cols_out_new,
        mean_rows[20:28],
        spreads[20:28],
        weight_scale[20:28],
    )
    cap_new, cap_copy, cap_update = apply_update(
        w_cap[None],
        grad_cap_all,
        rows_cap_new[None],
        cols_cap_new[None],
        mean_rows[28:29],
        spreads[28:29],
        weight_scale[28:29],
    )
    small_new, small_copy, small_update = apply_update(
        w_small[None],
        grad_small_all,
        rows_small_new[None],
        cols_small_new[None],
        mean_rows[29:30],
        spreads[29:30],
        weight_scale[29:30],
    )
    return (
        loss_total * inverse,
        in_new,
        in_copy,
        in_update,
        rows_in_new,
        cols_in_new,
        out_new,
        out_copy,
        out_update,
        rows_out_new,
        cols_out_new,
        cap_new[0],
        cap_copy[0],
        cap_update[0],
        rows_cap_new,
        cols_cap_new,
        small_new[0],
        small_copy[0],
        small_update[0],
        rows_small_new,
        cols_small_new,
        spreads,
    )


def solution(mesh):
    in_specs = (
        P("dp", None, None, None),
        P("dp", None, None, None),
        P("dp"),
        P("dp"),
        P("dp", None, None),
        P(None, "dp", None),
        P(None, "dp", None),
        P("dp", None),
        P(),
        P(None, "dp"),
        P(),
        P(None, "dp"),
        P(),
        P("dp"),
        P(),
        P(),
        P(),
    )
    out_specs = (
        P(),
        P(None, "dp", None),
        P(None, "dp", None),
        P(None, "dp", None),
        P(None, "dp"),
        P(),
        P(None, "dp", None),
        P(None, "dp", None),
        P(None, "dp", None),
        P(None, "dp"),
        P(),
        P("dp", None),
        P("dp", None),
        P("dp", None),
        P("dp"),
        P(),
        P(),
        P(),
        P(),
        P(),
        P(),
        P(),
    )
    return jax.shard_map(shards, mesh=mesh, in_specs=in_specs, out_specs=out_specs, check_vma=False)
```

```python
import math

import jax
import jax.numpy as jnp
from jax import lax
from jax.experimental import pallas as pl
from jax.experimental.pallas import tpu as pltpu
from jax.sharding import PartitionSpec as P

HEAD_DIM = 72
D = 1152
FREQ = 256
CAP_DIM = 4096
CAP_LEN = 120
FRAMES = 8
GRID_H = 4
GRID_W = 8
PATCHES = 32
SLOTS = 2
STEP = 20
TOK_DEV = 512
CAP_PAD = 128


norm_eps = 1e-06
relative_rate = 0.5
tanh_coeff = math.sqrt(2.0 / math.pi)
angle_unit = math.pi / 2.0 / 1.008 / 1000.0


def product(left, right):
    return jnp.dot(left, right, preferred_element_type=jnp.float32)


def contract(form, left, right):
    return jnp.einsum(form, left, right, preferred_element_type=jnp.float32)


def gelu_tanh(values):
    return (
        0.5 * values * (1.0 + jnp.tanh(tanh_coeff * (values + 0.044715 * values * values * values)))
    )


def layer_norm(values):
    center = values - jnp.mean(values, axis=-1, keepdims=True)
    return center * lax.rsqrt(jnp.mean(center * center, axis=-1, keepdims=True) + norm_eps)


def modulate(hidden, shift_rows, scale_rows):
    return layer_norm(hidden) * (1.0 + scale_rows) + shift_rows


def modulate_grad(hidden, shift_rows, scale_rows, grad_rows):
    pullback = jax.vjp(modulate, hidden, shift_rows, scale_rows)[1]
    return pullback(grad_rows)


def act_grad(function, values, grad_rows):
    return jax.vjp(function, values)[1](grad_rows)[0]


def sincos(positions, table_width):
    half_width = table_width // 2
    frequency = jnp.exp(
        -math.log(10000.0) * jnp.arange(half_width).astype(jnp.float32) / half_width
    )
    angles = positions[:, None] * frequency[None, :]
    return jnp.concatenate([jnp.sin(angles), jnp.cos(angles)], axis=1)


def position_tables():
    patch_index = jnp.arange(GRID_H * GRID_W)
    spatial = jnp.concatenate(
        [
            sincos((patch_index // GRID_W).astype(jnp.float32), D // 2),
            sincos((patch_index % GRID_W).astype(jnp.float32), D // 2),
        ],
        axis=1,
    )
    temporal = sincos(jnp.arange(FRAMES).astype(jnp.float32), D)
    return (spatial, temporal)


def time_features(timesteps):
    half_width = FREQ // 2
    frequency = jnp.exp(
        -math.log(10000.0) * jnp.arange(half_width).astype(jnp.float32) / half_width
    )
    angles = timesteps.astype(jnp.float32)[:, None] * frequency[None, :]
    return jnp.concatenate([jnp.cos(angles), jnp.sin(angles)], axis=1)


def plan(timesteps):
    moment = timesteps.astype(jnp.float32)
    start_angle = 8.0 * angle_unit
    cos_start = math.cos(start_angle) ** 2
    remain_now = jnp.sin((1000.0 - moment) * angle_unit)
    remain_before = jnp.sin((1001.0 - moment) * angle_unit)
    alpha_now = remain_now * remain_now / cos_start
    alpha_before = remain_before * remain_before / cos_start
    rest_now = (
        jnp.sin(2.0 * start_angle + moment * angle_unit) * jnp.sin(moment * angle_unit) / cos_start
    )
    rest_before = (
        jnp.sin(2.0 * start_angle + (moment - 1.0) * angle_unit)
        * jnp.sin((moment - 1.0) * angle_unit)
        / cos_start
    )
    beta_now = (
        jnp.sin(2.0 * start_angle + (2.0 * moment - 1.0) * angle_unit)
        * math.sin(angle_unit)
        / (remain_before * remain_before)
    )
    posterior = beta_now * rest_before / rest_now
    kappa = beta_now * beta_now * alpha_before / (rest_now * alpha_now)
    return (alpha_now, rest_now, beta_now, posterior, kappa)


def patch_terms(output, target, squared, beta_rows, posterior_rows, kappa_rows):
    error_rows = output[:, :, 0:4] - target
    log_beta = jnp.log(beta_rows)[:, None, None]
    log_post = jnp.log(posterior_rows)[:, None, None]
    fraction = (output[:, :, 4:8] + 1.0) * 0.5
    log_model = fraction * log_beta + (1.0 - fraction) * log_post
    diverge = 0.5 * (
        -1.0
        + log_model
        - log_post
        + jnp.exp(log_post - log_model)
        + kappa_rows[:, None, None] * squared * jnp.exp(-log_model)
    )
    return jnp.mean(error_rows * error_rows, axis=(1, 2)) + jnp.mean(
        diverge, axis=(1, 2)
    ) / math.log(2.0)


def to_frames(stacked, head_count):
    leading = stacked.shape[0]
    return (
        stacked.reshape(leading, SLOTS, FRAMES, PATCHES, head_count, HEAD_DIM)
        .transpose(0, 1, 3, 2, 4, 5)
        .reshape(leading, SLOTS * PATCHES, FRAMES, head_count, HEAD_DIM)
    )


def from_frames(stacked, head_count):
    leading = stacked.shape[0]
    return (
        stacked.reshape(leading, SLOTS, PATCHES, FRAMES, head_count, HEAD_DIM)
        .transpose(0, 1, 3, 2, 4, 5)
        .reshape(leading, SLOTS * FRAMES * PATCHES, head_count * HEAD_DIM)
    )


def attend_forward(queries, key_rows, value_rows):
    scores = contract("bqhc,bkhc->bhqk", queries, key_rows) * HEAD_DIM ** (-0.5)
    highest = jnp.max(scores, axis=-1, keepdims=True)
    shifted = jnp.exp(scores - highest)
    denominator = jnp.sum(shifted, axis=-1, keepdims=True)
    weights = (shifted / denominator).astype(jnp.bfloat16)
    return (contract("bhqk,bkhc->bqhc", weights, value_rows), highest + jnp.log(denominator))


def attend_backward(queries, key_rows, value_rows, logsum, grad_mixed):
    scores = contract("bqhc,bkhc->bhqk", queries, key_rows) * HEAD_DIM ** (-0.5)
    probability = jnp.exp(scores - logsum)
    grad_value = contract("bhqk,bqhc->bkhc", probability.astype(jnp.bfloat16), grad_mixed)
    grad_prob = contract("bqhc,bkhc->bhqk", grad_mixed, value_rows)
    grad_scores = (
        probability * (grad_prob - jnp.sum(probability * grad_prob, axis=-1, keepdims=True))
    ).astype(jnp.bfloat16)
    grad_query = contract("bhqk,bkhc->bqhc", grad_scores, key_rows) * HEAD_DIM ** (-0.5)
    grad_key = contract("bhqk,bqhc->bkhc", grad_scores, queries) * HEAD_DIM ** (-0.5)
    return (grad_query, grad_key, grad_value)


def new_stat(old_stat, sums, length, inverse_sq):
    rho = 1.0 - STEP ** (-0.8)
    return rho * old_stat + (1.0 - rho) * (sums * inverse_sq / length + 1e-30)


def ratio_terms(weight, grad, rows_new, cols_new):
    ratio = jnp.sum(grad * grad / (rows_new[:, :, None] * cols_new[:, None, :]), axis=(1, 2))
    return jnp.stack([jnp.sum(rows_new, axis=1), ratio, jnp.sum(weight * weight, axis=(1, 2))])


def apply_update(weight, grad, rows_new, cols_new, mean_rows, spread, weight_scale):
    second = rows_new[:, :, None] * cols_new[:, None, :] / mean_rows[:, None, None]
    update = grad * lax.rsqrt(second)
    clipped = update / jnp.maximum(1.0, spread)[:, None, None]
    new_weight = weight - relative_rate * weight_scale[:, None, None] * clipped
    return (new_weight, new_weight.astype(jnp.bfloat16), clipped)


MESH_ID = pl.DeviceIdType.MESH
ROW_STEP = 16


def remote(source, target, send_sem, recv_sem, device):
    return pltpu.make_async_remote_copy(
        src_ref=source,
        dst_ref=target,
        send_sem=send_sem,
        recv_sem=recv_sem,
        device_id=device,
        device_id_type=MESH_ID,
    )


def greet(devices):
    barrier = pltpu.get_barrier_semaphore()
    for device in devices:
        pl.semaphore_signal(barrier, inc=1, device_id=device, device_id_type=MESH_ID)
    pl.semaphore_wait(barrier, len(devices))


def exchange(axis, arrays, shared, number):
    size = lax.axis_size(axis)
    count = len(arrays)

    def kernel(*refs):
        sources, results = refs[0:count], refs[count : 2 * count]
        send_sem, recv_sem = refs[2 * count :]
        me = lax.axis_index(axis)
        peers = [lax.rem(me + step, size) for step in range(1, size)]
        greet([{axis: peer} for peer in peers])
        copies = []
        for step, peer in enumerate(peers):
            for at in range(count):
                source = sources[at] if shared[at] else sources[at].at[peer]
                copy = remote(
                    source,
                    results[at].at[me],
                    send_sem.at[at, step],
                    recv_sem.at[at, step],
                    {axis: peer},
                )
                copy.start()
                copies.append(copy)
        for at in range(count):
            own = sources[at][...] if shared[at] else sources[at][me]
            results[at][me] = own
        for copy in copies:
            copy.wait()

    shapes = [
        jax.ShapeDtypeStruct((size,) + (array.shape if keep else array.shape[1:]), array.dtype)
        for array, keep in zip(arrays, shared)
    ]
    vmem = pl.BlockSpec(memory_space=pltpu.VMEM)
    return pl.pallas_call(
        kernel,
        out_shape=shapes,
        in_specs=[vmem] * count,
        out_specs=[vmem] * count,
        scratch_shapes=[
            pltpu.SemaphoreType.DMA((count, size - 1)),
            pltpu.SemaphoreType.DMA((count, size - 1)),
        ],
        compiler_params=pltpu.CompilerParams(collective_id=number, has_side_effects=True),
        name=f"exchange_{axis}_{number}",
    )(*arrays)


def across(pieces, own, step_rows, row_types, sums, gather, number):
    size = lax.axis_size("mp")
    chips = size // 2
    adds = pieces is not None
    rows = pieces.shape[0] // size if adds else own[0].shape[0]
    width = own[0].shape[1] if own else pieces.shape[1]
    bfloat = jnp.bfloat16
    n_own, n_rows = len(own), len(row_types)

    def kernel(*refs):
        refs = list(refs)
        if adds:
            part = refs.pop(0)
        owns, refs = refs[0:n_own], refs[n_own:]
        row_refs, refs = refs[0:n_rows], refs[n_rows:]
        sum_refs, refs = refs[0:sums], refs[sums:]
        if gather:
            full = refs.pop(0)
        if adds:
            near, away, far, near_send, near_recv, far_send, far_recv = refs[0:7]
            refs = refs[7:]
        me = lax.axis_index("mp")
        core = lax.rem(me, 2)
        chip = me // 2
        partner = me + 1 - 2 * core

        def device(number_at):
            return {"mp": number_at}

        def at_step(step):
            return lax.rem(chip + step, chips)

        def block(number_at):
            return pl.ds(pl.multiple_of(number_at * rows, rows), rows)

        greet([device(partner)] + [device(at_step(k) * 2 + core) for k in range(1, chips)])
        pending = []
        if adds:
            near_copies = {}
            for k in list(range(1, chips)) + [0]:
                copy = remote(
                    part.at[block(at_step(k) * 2 + 1 - core)],
                    near.at[k],
                    near_send.at[k],
                    near_recv.at[k],
                    device(partner),
                )
                copy.start()
                near_copies[k] = copy
                pending.append(copy)
            far_copies = []
            for k in range(1, chips):
                near_copies[k].wait_recv()
                start = (at_step(k) * 2 + core) * rows

                @pl.loop(0, rows // ROW_STEP)
                def _(i):
                    here = pl.ds(pl.multiple_of(i * ROW_STEP, ROW_STEP), ROW_STEP)
                    there = pl.ds(pl.multiple_of(start + i * ROW_STEP, ROW_STEP), ROW_STEP)
                    away[k - 1, here] = (
                        part[there].astype(jnp.float32) + near[k, here].astype(jnp.float32)
                    ).astype(bfloat)

                copy = remote(
                    away.at[k - 1],
                    far.at[k - 1],
                    far_send.at[k - 1],
                    far_recv.at[k - 1],
                    device(at_step(k) * 2 + core),
                )
                copy.start()
                far_copies.append(copy)
                pending.append(copy)
            near_copies[0].wait_recv()
            for copy in far_copies:
                copy.wait_recv()
        for ref in sum_refs:
            ref[...] = jnp.zeros_like(ref)
        mine = me * rows

        @pl.loop(0, rows // ROW_STEP)
        def _(i):
            here = pl.ds(pl.multiple_of(i * ROW_STEP, ROW_STEP), ROW_STEP)
            there = pl.ds(pl.multiple_of(mine + i * ROW_STEP, ROW_STEP), ROW_STEP)
            values = [ref[here] if ref.shape[0] == rows else ref[...] for ref in owns]
            if adds:
                total = part[there].astype(jnp.float32) + near[0, here].astype(jnp.float32)
                for k in range(1, chips):
                    total = total + far[k - 1, here].astype(jnp.float32)
                row_values, terms, sent = step_rows(total, *values)
            else:
                row_values, terms, sent = [], [], values[0]
            for ref, value in zip(row_refs, row_values):
                ref[here] = value.astype(ref.dtype)
            for ref, value in zip(sum_refs, terms):
                ref[...] += jnp.sum(value.reshape(ROW_STEP // 8, 8, width), axis=0)
            if gather:
                full[there] = sent.astype(bfloat)

        if gather:
            out_send, out_recv, back_send, back_recv = refs
            outward = []
            for k in list(range(1, chips)) + [0]:
                copy = remote(
                    full.at[block(me)],
                    full.at[block(me)],
                    out_send.at[k],
                    out_recv.at[k],
                    device(at_step(k) * 2 + core) if k else device(partner),
                )
                copy.start()
                outward.append(copy)
                pending.append(copy)
            backward = []
            for k in range(1, chips):
                outward[k - 1].wait_recv()
                came = at_step(chips - k) * 2 + core
                copy = remote(
                    full.at[block(came)],
                    full.at[block(came)],
                    back_send.at[k - 1],
                    back_recv.at[k - 1],
                    device(partner),
                )
                copy.start()
                backward.append(copy)
                pending.append(copy)
            outward[-1].wait_recv()
            for copy in backward:
                copy.wait_recv()
        for copy in pending:
            copy.wait_send()

    dma = pltpu.SemaphoreType.DMA
    shapes = [jax.ShapeDtypeStruct((rows, width), kind) for kind in row_types]
    shapes += [jax.ShapeDtypeStruct((8, width), jnp.float32)] * sums
    scratch = []
    if gather:
        shapes.append(jax.ShapeDtypeStruct((rows * size, width), bfloat))
    if adds:
        scratch += [
            pltpu.VMEM((chips, rows, width), bfloat),
            pltpu.VMEM((chips - 1, rows, width), bfloat),
            pltpu.VMEM((chips - 1, rows, width), bfloat),
            dma((chips,)),
            dma((chips,)),
            dma((chips - 1,)),
            dma((chips - 1,)),
        ]
    if gather:
        scratch += [dma((chips,)), dma((chips,)), dma((chips - 1,)), dma((chips - 1,))]
    vmem = pl.BlockSpec(memory_space=pltpu.VMEM)
    inputs = ([pieces] if adds else []) + list(own)
    return pl.pallas_call(
        kernel,
        out_shape=shapes,
        in_specs=[vmem] * len(inputs),
        out_specs=[vmem] * len(shapes),
        scratch_shapes=scratch,
        compiler_params=pltpu.CompilerParams(collective_id=number, has_side_effects=True),
        name=f"across_{number}",
    )(*inputs)


def normalize(values):
    center = values - jnp.mean(values, axis=-1, keepdims=True)
    spread = lax.rsqrt(jnp.mean(center * center, axis=-1, keepdims=True) + norm_eps)
    return center * spread, spread


def normalize_grad(normal, spread, grad_rows):
    mean_grad = jnp.mean(grad_rows, axis=-1, keepdims=True)
    mean_both = jnp.mean(grad_rows * normal, axis=-1, keepdims=True)
    return spread * (grad_rows - mean_grad - normal * mean_both)


def pad_samples(rows):
    stacked = rows.reshape(SLOTS, CAP_LEN, rows.shape[1])
    padded = jnp.pad(stacked, ((0, 0), (0, CAP_PAD - CAP_LEN), (0, 0)))
    return padded.reshape(SLOTS * CAP_PAD, rows.shape[1])


def cut_samples(rows):
    stacked = rows.reshape(SLOTS, CAP_PAD, rows.shape[1])[:, 0:CAP_LEN]
    return stacked.reshape(SLOTS * CAP_LEN, rows.shape[1])


def side_by_side(stacked):
    return stacked.transpose(1, 0, 2).reshape(stacked.shape[1], -1)


def heads_of(rows, lead, count):
    return rows.reshape(*lead, count, HEAD_DIM)


def spatial_heads(rows, count):
    return rows.reshape(SLOTS * FRAMES, PATCHES, count, HEAD_DIM)


def temporal_heads(rows, count):
    return to_frames(rows[None], count)[0]


def shards(
    latents, gaussian_noise, timesteps, counts, captions,
    w_in, w_out, w_cap, w_small,
    rows_in, cols_in, rows_out, cols_out, rows_cap, cols_cap, rows_small, cols_small,
):
    bfloat = jnp.bfloat16
    mp_index = lax.axis_index("mp")
    dp_index = lax.axis_index("dp")
    mp_size = lax.axis_size("mp")
    dp_size = lax.axis_size("dp")
    local_width = w_in.shape[2] // mp_size
    head_count = local_width // HEAD_DIM
    col_start = mp_index * local_width
    row_count_own = w_in.shape[1]
    row_start = dp_index * row_count_own
    cap_rows_own = w_cap.shape[0]
    small_rows = 56 + FREQ
    per_sample = FRAMES * PATCHES
    own_tokens = TOK_DEV // mp_size
    token_start = mp_index * own_tokens
    sample = token_start // per_sample
    wide = 4 * local_width
    lw = local_width

    in_cols = lax.dynamic_slice_in_dim(w_in[0:13], col_start, lw, 2).astype(bfloat)
    out_cols = lax.dynamic_slice_in_dim(w_out, col_start, lw, 2).astype(bfloat)
    cap_cols = lax.dynamic_slice_in_dim(w_cap, col_start, lw, 1).astype(bfloat)
    pack_s = side_by_side(jnp.concatenate([in_cols[0:3], out_cols[0:1]], axis=0))
    pack_t = side_by_side(jnp.concatenate([in_cols[3:6], out_cols[1:2]], axis=0))
    pack_c = side_by_side(jnp.concatenate([in_cols[6:9], out_cols[2:3]], axis=0))
    pack_i = side_by_side(in_cols[9:13])
    pack_o = side_by_side(out_cols[3:7])
    pack_x = jnp.concatenate([cap_cols, out_cols[7]], axis=0)
    full_s = lax.all_gather(pack_s, "dp", axis=0, tiled=True)
    full_t = lax.all_gather(pack_t, "dp", axis=0, tiled=True)
    full_x = lax.all_gather(pack_x, "dp", axis=0, tiled=False)
    full_c = lax.all_gather(pack_c, "dp", axis=0, tiled=True)
    full_i = lax.all_gather(pack_i, "dp", axis=0, tiled=True)
    full_o = lax.all_gather(pack_o, "dp", axis=0, tiled=True)
    full_cap = full_x[:, 0:cap_rows_own].reshape(CAP_DIM, lw)
    full_c2 = full_x[:, cap_rows_own:].reshape(D, lw)
    mod_rows = w_in[13:19].astype(bfloat)
    temb_rows = w_in[19].astype(bfloat)

    full_small = w_small.astype(bfloat)
    patch_w = full_small[0:16]
    freq_w = full_small[16 : 16 + FREQ]
    tables = full_small[16 + FREQ : 24 + FREQ].astype(jnp.float32)
    final_w = full_small[24 + FREQ :]

    def own_rows(rows):
        return lax.dynamic_slice_in_dim(rows, token_start, own_tokens, 0)

    def own_cols(rows):
        return lax.dynamic_slice_in_dim(rows, row_start, row_count_own, 1)

    numbers = jnp.zeros((8, 128), jnp.int32)
    numbers = numbers.at[0, 0:SLOTS].set(timesteps).at[0, SLOTS].set(counts[0])
    numbers_all = exchange("dp", [numbers], [True], 1)[0]
    all_times = numbers_all[:, 0, 0:SLOTS].reshape(-1)
    count_total = jnp.sum(numbers_all[:, 0, SLOTS]).astype(jnp.float32)
    alpha_now, rest_now, beta_now, posterior, kappa = plan(timesteps)
    features = time_features(all_times).astype(bfloat)
    first_pre = product(features, freq_w)
    first_act = jax.nn.silu(first_pre).astype(bfloat)
    temb_part = product(own_cols(first_act), temb_rows)
    sample_count = temb_part.shape[0]
    temb_cols_all, temb_rows_all = exchange(
        "dp",
        [
            temb_part.reshape(sample_count, dp_size, row_count_own).transpose(1, 0, 2),
            temb_part.reshape(dp_size, SLOTS, D),
        ],
        [False, False],
        2,
    )
    time_cols = jnp.sum(temb_cols_all, axis=0)
    time_emb = jnp.sum(temb_rows_all, axis=0)
    temb_act = jax.nn.silu(time_cols).astype(bfloat)
    mod_part = contract("sd,kde->ske", temb_act, mod_rows)
    modulation = (
        jnp.sum(exchange("dp", [mod_part.reshape(dp_size, SLOTS * 6, D)], [False], 3)[0], axis=0)
        .reshape(SLOTS, 6, D)
        + tables[None, 0:6]
    )
    mods_own = lax.dynamic_index_in_dim(modulation, sample, 0, keepdims=False)
    shift_a, scale_a, gate_a, shift_b, scale_b, gate_b = [
        mods_own[number : number + 1] for number in range(6)
    ]
    temb_own = lax.dynamic_slice_in_dim(time_emb, sample, 1, 0)

    noisy_low = (
        jnp.sqrt(alpha_now)[:, None, None, None] * latents.astype(jnp.float32)
        + jnp.sqrt(rest_now)[:, None, None, None] * gaussian_noise
    ).astype(bfloat)
    patches = noisy_low.reshape(TOK_DEV, 16)
    spatial_pos, temporal_pos = position_tables()
    start_hidden = (
        product(patches, patch_w).reshape(SLOTS * FRAMES, PATCHES, D) + spatial_pos[None]
    ).reshape(SLOTS, per_sample, D)
    start_own = own_rows(start_hidden.reshape(TOK_DEV, D))

    cap_rows = captions.reshape(SLOTS * CAP_LEN, CAP_DIM)
    cap_mid = product(cap_rows, full_cap)
    cap_act = gelu_tanh(cap_mid).astype(bfloat)
    context_part = pad_samples(contract("re,de->rd", cap_act, full_c2).astype(bfloat))
    context_low = cut_samples(
        across(context_part, [], lambda total: ([], [], total), [], 0, True, 4)[0]
    )

    normed_a = (
        modulate(start_hidden, modulation[:, 0][:, None], modulation[:, 1][:, None])
        .astype(bfloat)
        .reshape(TOK_DEV, D)
    )
    qkv = product(normed_a, full_s[:, 0 : 3 * lw]).astype(bfloat)
    qkv_s = [spatial_heads(qkv[:, k * lw : (k + 1) * lw], head_count) for k in range(3)]
    mixed_s, logsum_s = attend_forward(*qkv_s)
    mixed_s_low = mixed_s.astype(bfloat).reshape(TOK_DEV, lw)
    frame_start = (token_start % per_sample) // PATCHES
    frames_own = own_tokens // PATCHES
    temporal_own = lax.dynamic_slice_in_dim(temporal_pos, frame_start, frames_own, 0)
    temporal_rows = jnp.broadcast_to(
        temporal_own[:, None, :], (frames_own, PATCHES, D)
    ).reshape(own_tokens, D)

    def spatial_step(total, start_rows, gate, position):
        hidden = start_rows + gate * total
        return [total, hidden], [], hidden + position

    f32 = jnp.float32
    branch_s, hidden_s, timed_low = across(
        contract("te,de->td", mixed_s_low, full_s[:, 3 * lw :]).astype(bfloat),
        [start_own, gate_a, temporal_rows],
        spatial_step,
        [f32, f32],
        0,
        True,
        5,
    )
    qkv = product(timed_low, full_t[:, 0 : 3 * lw]).astype(bfloat)
    qkv_t = [temporal_heads(qkv[:, k * lw : (k + 1) * lw], head_count) for k in range(3)]
    mixed_t, logsum_t = attend_forward(*qkv_t)
    mixed_t_low = from_frames(mixed_t.astype(bfloat)[None], head_count)[0]

    def temporal_step(total, hidden_rows, gate):
        hidden = hidden_rows + gate * total
        return [total, hidden], [], hidden

    branch_t, hidden_t, hidden_low = across(
        contract("te,de->td", mixed_t_low, full_t[:, 3 * lw :]).astype(bfloat),
        [hidden_s, gate_a],
        temporal_step,
        [f32, f32],
        0,
        True,
        6,
    )
    query_c = (
        product(hidden_low, full_c[:, 0:lw])
        .astype(bfloat)
        .reshape(SLOTS, per_sample, head_count, HEAD_DIM)
    )
    key_value = product(context_low, full_c[:, lw : 3 * lw]).astype(bfloat)
    key_c = key_value[:, 0:lw].reshape(SLOTS, CAP_LEN, head_count, HEAD_DIM)
    value_c = key_value[:, lw:].reshape(SLOTS, CAP_LEN, head_count, HEAD_DIM)
    mixed_c, logsum_c = attend_forward(query_c, key_c, value_c)
    mixed_c_low = mixed_c.astype(bfloat).reshape(TOK_DEV, lw)

    def cross_step(total, hidden_rows, shift, scale):
        hidden = hidden_rows + total
        return [hidden], [], normalize(hidden)[0] * (1.0 + scale) + shift

    hidden_c, normed_b = across(
        contract("te,de->td", mixed_c_low, full_c[:, 3 * lw :]).astype(bfloat),
        [hidden_t, shift_b, scale_b],
        cross_step,
        [f32],
        0,
        True,
        7,
    )
    inner_pre = product(normed_b, full_i)
    inner_act = gelu_tanh(inner_pre).astype(bfloat)
    shift_f = tables[6:7] + temb_own
    scale_f = tables[7:8] + temb_own

    def forward_step(total, hidden_rows, gate, shift, scale):
        hidden = hidden_rows + gate * total
        return [total, hidden, normalize(hidden)[0] * (1.0 + scale) + shift], [], None

    branch_m, hidden_m, normed_f = across(
        contract("te,de->td", inner_act, full_o).astype(bfloat),
        [hidden_c, gate_b, shift_f, scale_f],
        forward_step,
        [f32, f32, bfloat],
        0,
        False,
        8,
    )
    output = contract("td,od->to", normed_f, final_w).reshape(own_tokens, 4, 8)
    target = own_rows(gaussian_noise.reshape(TOK_DEV, 4, 4))
    error_rows = output[:, :, 0:4] - target
    squared = error_rows * error_rows
    live = (sample * per_sample < counts[0]).astype(jnp.float32)

    def of_sample(values):
        return jnp.broadcast_to(lax.dynamic_slice_in_dim(values, sample, 1, 0), (own_tokens,))

    beta_rows = of_sample(beta_now)
    posterior_rows = of_sample(posterior)
    kappa_rows = of_sample(kappa)

    def patch_loss(values):
        return jnp.sum(
            patch_terms(values, target, squared, beta_rows, posterior_rows, kappa_rows) * live
        )

    loss_local, loss_pull = jax.vjp(patch_loss, output)
    grad_output = loss_pull(jnp.ones_like(loss_local))[0].astype(bfloat).reshape(own_tokens, 32)
    grad_final = contract("to,td->od", grad_output, normed_f)
    grad_normed = contract("to,od->td", grad_output, final_w)
    grad_hidden, grad_shift_f, grad_scale_f = modulate_grad(hidden_m, shift_f, scale_f, grad_normed)
    grad_gate_b = jnp.sum(grad_hidden * branch_m, axis=0, keepdims=True)
    grad_branch = across(
        None, [(gate_b * grad_hidden).astype(bfloat)], None, [], 0, True, 9
    )[0]
    grad_inner = act_grad(gelu_tanh, inner_pre, product(grad_branch, full_o)).astype(bfloat)
    part = contract("te,de->td", grad_inner, full_i)
    grad_pack_o = contract("td,te->de", grad_branch, inner_act)
    grad_pack_i = contract("td,te->de", normed_b, grad_inner)

    def row_sum(pieces):
        return lax.psum_scatter(
            pieces.astype(bfloat), "dp", scatter_dimension=0, tiled=True
        )

    sum_o = row_sum(grad_pack_o)
    sum_i = row_sum(grad_pack_i)

    def forward_grad_step(total, hidden_rows, scale, grad_rows):
        normal, spread = normalize(hidden_rows)
        grad = grad_rows + normalize_grad(normal, spread, total * (1.0 + scale))
        return [grad], [total, total * normal], grad

    def one_row(rows):
        return jnp.sum(rows, axis=0, keepdims=True)

    grad_hidden, grad_shift_b, grad_scale_b, grad_branch = across(
        part.astype(bfloat),
        [hidden_c, scale_b, grad_hidden],
        forward_grad_step,
        [f32],
        2,
        True,
        10,
    )
    grad_mixed = (
        product(grad_branch, full_c[:, 3 * lw :])
        .astype(bfloat)
        .reshape(SLOTS, per_sample, head_count, HEAD_DIM)
    )
    grad_query, grad_key, grad_value = attend_backward(
        query_c, key_c, value_c, logsum_c, grad_mixed
    )
    grad_query = grad_query.astype(bfloat).reshape(TOK_DEV, lw)
    grad_kv = jnp.concatenate(
        [
            grad_key.astype(bfloat).reshape(SLOTS * CAP_LEN, lw),
            grad_value.astype(bfloat).reshape(SLOTS * CAP_LEN, lw),
        ],
        axis=1,
    )
    part = contract("te,de->td", grad_query, full_c[:, 0:lw])
    part_context = contract("re,de->rd", grad_kv, full_c[:, lw : 3 * lw])
    sum_c = row_sum(
        jnp.concatenate(
            [
                contract("td,te->de", hidden_low, grad_query),
                contract("rd,re->de", context_low, grad_kv),
                contract("td,te->de", grad_branch, mixed_c_low),
            ],
            axis=1,
        )
    )

    def gated_step(total, grad_rows, branch_rows, gate):
        grad = grad_rows + total
        return [grad], [grad * branch_rows], gate * grad

    grad_hidden, grad_gate_t, grad_branch = across(
        part.astype(bfloat), [grad_hidden, branch_t, gate_a], gated_step, [f32], 1, True, 11
    )
    grad_mixed = temporal_heads(
        product(grad_branch, full_t[:, 3 * lw :]).astype(bfloat), head_count
    )
    grads_t = attend_backward(*qkv_t, logsum_t, grad_mixed)
    grad_qkv = from_frames(jnp.stack(grads_t).astype(bfloat), head_count)
    grad_qkv = jnp.concatenate([grad_qkv[0], grad_qkv[1], grad_qkv[2]], axis=1)
    part = contract("te,de->td", grad_qkv, full_t[:, 0 : 3 * lw])
    sum_t = row_sum(
        jnp.concatenate(
            [
                contract("td,te->de", timed_low, grad_qkv),
                contract("td,te->de", grad_branch, mixed_t_low),
            ],
            axis=1,
        )
    )
    grad_hidden, grad_gate_s, grad_branch = across(
        part.astype(bfloat), [grad_hidden, branch_s, gate_a], gated_step, [f32], 1, True, 12
    )
    grad_mixed = spatial_heads(
        product(grad_branch, full_s[:, 3 * lw :]).astype(bfloat), head_count
    )
    grads_s = attend_backward(*qkv_s, logsum_s, grad_mixed)
    grad_qkv = jnp.concatenate(
        [grad.astype(bfloat).reshape(TOK_DEV, lw) for grad in grads_s], axis=1
    )
    part = contract("te,de->td", grad_qkv, full_s[:, 0 : 3 * lw])
    sum_s = row_sum(
        jnp.concatenate(
            [
                contract("td,te->de", normed_a, grad_qkv),
                contract("td,te->de", grad_branch, mixed_s_low),
            ],
            axis=1,
        )
    )
    grad_context = cut_samples(
        across(
            pad_samples(part_context.astype(bfloat)),
            [],
            lambda total: ([], [], total),
            [],
            0,
            True,
            13,
        )[0]
    )
    grad_cap2 = contract("rd,re->de", grad_context, cap_act)
    grad_cap_mid = act_grad(
        gelu_tanh, cap_mid, contract("rd,de->re", grad_context, full_c2)
    ).astype(bfloat)
    grad_cap = contract("rc,re->ce", cap_rows, grad_cap_mid)
    sum_x = row_sum(
        jnp.concatenate(
            [
                grad_cap.reshape(dp_size, cap_rows_own, lw),
                grad_cap2.reshape(dp_size, row_count_own, lw),
            ],
            axis=1,
        ).reshape(dp_size * (cap_rows_own + row_count_own), lw)
    )

    def start_grad_step(total, hidden_rows, scale, grad_rows):
        normal, spread = normalize(hidden_rows)
        grad = grad_rows + normalize_grad(normal, spread, total * (1.0 + scale))
        return [grad], [total, total * normal], None

    grad_start, grad_shift_a, grad_scale_a = across(
        part.astype(bfloat),
        [start_own, scale_a, grad_hidden],
        start_grad_step,
        [bfloat],
        2,
        False,
        14,
    )
    grad_patch = contract("ti,td->id", own_rows(patches), grad_start)
    grad_mods = jnp.concatenate(
        [
            one_row(grad_shift_a), one_row(grad_scale_a), one_row(grad_gate_t + grad_gate_s),
            one_row(grad_shift_b), one_row(grad_scale_b), grad_gate_b,
            grad_shift_f, grad_scale_f,
        ],
        axis=0,
    )
    placed = jnp.where(
        (jnp.arange(SLOTS) == sample)[:, None, None], grad_mods[None], 0.0
    ).reshape(SLOTS * 8, D)
    small_rows_part = jnp.concatenate([grad_patch, grad_final], axis=0)
    small_count = small_rows_part.shape[0] // mp_size
    loss_block = jnp.broadcast_to(loss_local, (8, 128))
    placed_all, small_all, loss_all = exchange(
        "mp",
        [placed, small_rows_part.reshape(mp_size, small_count, D), loss_block],
        [True, False, True],
        15,
    )
    grad_mods = jnp.sum(placed_all, axis=0).reshape(SLOTS, 8, D)
    small_own = jnp.sum(small_all, axis=0).astype(bfloat)
    loss_part = jnp.sum(loss_all[:, 0, 0])
    mods_all, small_all = exchange(
        "dp", [grad_mods.astype(bfloat).reshape(SLOTS * 8, D), small_own], [True, True], 16
    )
    mods_all = mods_all.reshape(dp_size * SLOTS, 8, D)
    small_own = jnp.sum(small_all.astype(f32), axis=0)
    grad_mods_low = mods_all[:, 0:6]
    grad_tables = jnp.sum(mods_all.astype(f32), axis=0)
    grad_temb_act = contract("ske,kde->sd", grad_mods_low, mod_rows)
    grad_temb = act_grad(jax.nn.silu, time_cols, grad_temb_act) + own_cols(
        (mods_all[:, 6].astype(f32) + mods_all[:, 7].astype(f32))
    )

    def dp_columns(rows, number):
        blocks = exchange("dp", [rows], [True], number)[0]
        return blocks.transpose(1, 0, 2).reshape(rows.shape[0], D)

    grad_temb_low = dp_columns(grad_temb.astype(bfloat), 17)
    grad_first_own = act_grad(
        jax.nn.silu, own_cols(first_pre), contract("sd,id->si", grad_temb_low, temb_rows)
    ).astype(bfloat)
    grad_first = dp_columns(grad_first_own, 18)
    grad_time = contract("sd,ske->kde", temb_act, grad_mods_low)
    grad_temb_part = contract("si,sd->id", own_cols(first_act), grad_temb_low)
    grad_freq = contract("sf,sd->fd", features, grad_first)
    small_part = exchange("mp", [small_own], [True], 19)[0].reshape(mp_size * small_count, D)
    sum_small = jnp.concatenate([small_part[0:16], grad_freq, grad_tables, small_part[16:]], axis=0)

    def all_columns(rows, number):
        blocks = exchange("mp", [rows], [True], number)[0]
        kinds = rows.shape[1] // lw
        stacked = blocks.reshape(mp_size, rows.shape[0], kinds, lw)
        return stacked.transpose(2, 1, 0, 3).reshape(kinds, rows.shape[0], mp_size * lw)

    whole_s, whole_t, whole_c, whole_i, whole_o, whole_x = [
        all_columns(rows, 22 + at).astype(jnp.float32)
        for at, rows in enumerate((sum_s, sum_t, sum_c, sum_i, sum_o, sum_x))
    ]
    sum_in = jnp.concatenate(
        [whole_s[0:3], whole_t[0:3], whole_c[0:3], whole_i, grad_time, grad_temb_part[None]], axis=0
    )
    sum_out = jnp.concatenate(
        [whole_s[3:4], whole_t[3:4], whole_c[3:4], whole_o, whole_x[:, cap_rows_own:]], axis=0
    )
    sum_cap = whole_x[0, 0:cap_rows_own]
    square_in = sum_in * sum_in
    square_out = sum_out * sum_out
    square_cap = sum_cap * sum_cap
    square_small = sum_small * sum_small
    row_in_total = jnp.sum(square_in, axis=2)
    row_out_total = jnp.sum(square_out, axis=2)
    row_cap_total = jnp.sum(square_cap, axis=1)
    row_small_total = jnp.sum(square_small, axis=1)
    col_small_total = jnp.sum(square_small, axis=0)
    col_part = jnp.concatenate(
        [
            jnp.sum(square_in, axis=1),
            jnp.sum(square_out, axis=1),
            jnp.sum(square_cap, axis=0, keepdims=True),
        ],
        axis=0,
    )
    col_all = exchange("dp", [col_part.astype(bfloat)], [True], 20)[0]
    col_total = jnp.sum(col_all.astype(f32), axis=0)
    col_in_total, col_out_total, col_cap_total = col_total[0:20], col_total[20:28], col_total[28]
    inverse = 1.0 / count_total
    inverse_sq = inverse * inverse
    rows_in_new = new_stat(rows_in, row_in_total, D, inverse_sq)
    cols_in_new = new_stat(cols_in, col_in_total, D, inverse_sq)
    rows_out_new = new_stat(rows_out, row_out_total, D, inverse_sq)
    cols_out_new = new_stat(cols_out, col_out_total, D, inverse_sq)
    rows_cap_new = new_stat(rows_cap, row_cap_total, D, inverse_sq)
    cols_cap_new = new_stat(cols_cap, col_cap_total, CAP_DIM, inverse_sq)
    rows_small_new = new_stat(rows_small, row_small_total, D, inverse_sq)
    cols_small_new = new_stat(cols_small, col_small_total, small_rows, inverse_sq)
    grad_in = sum_in * inverse
    grad_out = sum_out * inverse
    grad_cap_all = (sum_cap * inverse)[None]
    grad_small_all = (sum_small * inverse)[None]
    ratio_part = jnp.concatenate(
        [
            ratio_terms(w_in, grad_in, rows_in_new, cols_in_new),
            ratio_terms(w_out, grad_out, rows_out_new, cols_out_new),
            ratio_terms(w_cap[None], grad_cap_all, rows_cap_new[None], cols_cap_new[None]),
        ],
        axis=1,
    )
    ratio_block = jnp.zeros((8, 128), f32).at[0:3, 0:29].set(ratio_part).at[3, 0].set(loss_part)
    ratio_block = jnp.sum(exchange("dp", [ratio_block], [True], 21)[0], axis=0)
    ratios = ratio_block[0:3, 0:29]
    loss_total = ratio_block[3, 0]
    totals = jnp.concatenate(
        [
            ratios,
            ratio_terms(w_small[None], grad_small_all, rows_small_new[None], cols_small_new[None]),
        ],
        axis=1,
    )
    row_count = jnp.array([float(D)] * 28 + [float(CAP_DIM), float(small_rows)], jnp.float32)
    mean_rows = totals[0] / row_count
    spreads = jnp.sqrt(mean_rows * totals[1] / (row_count * D))
    weight_scale = jnp.sqrt(totals[2] / (row_count * D))
    in_new, in_copy, in_update = apply_update(
        w_in, grad_in, rows_in_new, cols_in_new, mean_rows[0:20], spreads[0:20], weight_scale[0:20]
    )
    out_new, out_copy, out_update = apply_update(
        w_out,
        grad_out,
        rows_out_new,
        cols_out_new,
        mean_rows[20:28],
        spreads[20:28],
        weight_scale[20:28],
    )
    cap_new, cap_copy, cap_update = apply_update(
        w_cap[None],
        grad_cap_all,
        rows_cap_new[None],
        cols_cap_new[None],
        mean_rows[28:29],
        spreads[28:29],
        weight_scale[28:29],
    )
    small_new, small_copy, small_update = apply_update(
        w_small[None],
        grad_small_all,
        rows_small_new[None],
        cols_small_new[None],
        mean_rows[29:30],
        spreads[29:30],
        weight_scale[29:30],
    )
    return (
        loss_total * inverse,
        in_new,
        in_copy,
        in_update,
        rows_in_new,
        cols_in_new,
        out_new,
        out_copy,
        out_update,
        rows_out_new,
        cols_out_new,
        cap_new[0],
        cap_copy[0],
        cap_update[0],
        rows_cap_new,
        cols_cap_new,
        small_new[0],
        small_copy[0],
        small_update[0],
        rows_small_new,
        cols_small_new,
        spreads,
    )


def solution(mesh):
    in_specs = (
        P("dp", None, None, None),
        P("dp", None, None, None),
        P("dp"),
        P("dp"),
        P("dp", None, None),
        P(None, "dp", None),
        P(None, "dp", None),
        P("dp", None),
        P(),
        P(None, "dp"),
        P(),
        P(None, "dp"),
        P(),
        P("dp"),
        P(),
        P(),
        P(),
    )
    out_specs = (
        P(),
        P(None, "dp", None),
        P(None, "dp", None),
        P(None, "dp", None),
        P(None, "dp"),
        P(),
        P(None, "dp", None),
        P(None, "dp", None),
        P(None, "dp", None),
        P(None, "dp"),
        P(),
        P("dp", None),
        P("dp", None),
        P("dp", None),
        P("dp"),
        P(),
        P(),
        P(),
        P(),
        P(),
        P(),
        P(),
    )
    return jax.shard_map(shards, mesh=mesh, in_specs=in_specs, out_specs=out_specs, check_vma=False)
```
